128 devices in a mesh: aa: 8 (over x, core), ba: 16 (over z, y).
Axes of the slice: x: 4, y: 4, z: 4, core: 2. Of those that a mesh axis runs over, the one named last changes fastest.
Arguments:
- head_outputs: bfloat16 [2048, 4096], P('ba'), may hold values from -6 to 6
- stream: bfloat16 [2048, 4096], P('ba'), may hold values from -6 to 6
- adapter_down_factors: bfloat16 [4096, 1024], P(None, 'aa'), may hold values from -0.09375 to 0.09375
- adapter_up_factors: bfloat16 [1024, 4096], P('aa'), may hold values from -1.5 to 1.5
- norm_gain_vector: float32 [4096], replicated, may hold values from 0.5 to 1.5
- router_matrix: bfloat16 [4096, 8], replicated, may hold values from -0.09375 to 0.09375
- token_adapter_index: int32 [2048], P('ba'), may hold values from 0 to 63
- token_expert_index: int32 [2048, 2], P('ba'), may hold values from 0 to 7, all different within a row; in each aligned block of 128 rows (0 to 127, 128 to 255, ...) at most 48 rows name the same one
- gate_weight: bfloat16 [16, 4096, 7168], P('ba', None, 'aa'), may hold values from -0.09375 to 0.09375
- up_weight: bfloat16 [16, 4096, 7168], P('ba', None, 'aa'), may hold values from -0.09375 to 0.09375
- down_weight: bfloat16 [16, 7168, 4096], P('ba', 'aa'), may hold values from -0.046875 to 0.046875
Outputs:
- mixed: bfloat16 [2048, 4096], P('ba', 'aa')
- adapter_load: float32 [64], P('aa')
The draws below stay inside these ranges and needn't reach their ends.
Inputs may be any that keep to these rules, and one draw needn't show every extreme that they name: `token_expert_index`: the two experts of a row differ; in each aligned block of 128 rows no expert is named by more than 48 rows.
All inputs are finite; a program needn't handle non-finite values.
Results may differ from the reference program's by a relative error of at most 0.0049.
Values may be sent and summed in bfloat16 or wider, within the bound.
A program may use at most 128 MiB of HBM per device.

```python
import math
import jax
import jax.numpy as jnp
import numpy as np
from jax import lax

MODEL_DIM = 4096
FF = 14336
E = 8
ADAPTER_RANK = 16
TOK_DEV = 128
CAP = 48
TOKENS = 2048
ADAPTER_COUNT = 64
SLOTS = 16
SLOT_FF = 7168
N_BA = 16


def plant(drawn, stream_key, smallest, top_value):
    longest = drawn.shape.index(max(drawn.shape))
    spots = []
    for shift in (0, 1):
        where = [jax.random.randint(jax.random.fold_in(stream_key, axis), (), 0, length) for axis, length in enumerate(drawn.shape)]
        where[longest] = (where[longest] + shift) % drawn.shape[longest]
        spots.append(tuple(where))
    return drawn.at[spots[0]].set(smallest).at[spots[1]].set(top_value)


def shard_levels(rng, shape, split, smallest, high):
    factor_of = 1.0
    for dim, shards_of in split:
        heights = jax.random.uniform(jax.random.fold_in(jax.random.fold_in(rng, 6), dim), (shards_of,), jnp.float32, smallest / len(split), high / len(split))
        factor_of = factor_of * jnp.repeat(jnp.exp(heights), shape[dim] // shards_of).reshape((-1,) + (1,) * (len(shape) - 1 - dim))
    return factor_of


def rank_bounds(count, lean):
    loads = [(1 << 20) // math.isqrt(rank ** lean) + 1 for rank in range(1, count + 1)]
    deviation = 1 + sum(loads) // (1 << 30)
    return np.cumsum(np.array([max(1, weight // deviation) for weight in loads]))


def skewed_ids(own_key, extent, amount, slope):
    table = rank_bounds(amount, slope)
    lot = jax.random.randint(jax.random.fold_in(own_key, 1), extent, 0, int(table[amount - 1]))
    rank = jnp.searchsorted(jnp.asarray(table, jnp.int32), lot, side="right")
    return jax.random.permutation(jax.random.fold_in(own_key, 2), amount)[rank].astype(jnp.int32)


def deal_out(stream_key, own, number, rows, count, top, most, skew):
    sequence = jax.random.permutation(stream_key, count)
    heavy_load, ordinary = portions_of(count, rows * top, most, skew, True), portions_of(count, rows * top, most, skew, False)
    places = jnp.arange(count)

    def named(lengths, turn):
        used = int((lengths > 0).sum())
        fixed = max(1, used // 4)
        shifted = fixed + (places - fixed + turn * (used - fixed)) % max(1, count - fixed)
        return jnp.zeros((count,), jnp.int32).at[sequence[jnp.where(places < fixed, places, shifted)]].set(jnp.asarray(lengths, jnp.int32))

    lengths = jnp.where(number % 4 == 0, named(heavy_load, number // 4), named(ordinary, number - number // 4 - 1))
    mixed = jax.random.permutation(jax.random.fold_in(own, 3), count)
    giver, taker = mixed[0:count // 2 * 2:2], mixed[1:count // 2 * 2:2]
    margin = jnp.minimum(lengths[giver] - 1, most - lengths[taker]) // 2
    margin = jnp.where((giver == sequence[0]) | (taker == sequence[0]) | (lengths[taker] == 0), 0, jnp.maximum(margin, 0))
    shifted = jax.random.randint(jax.random.fold_in(own, 4), (count // 2,), 0, 1 << 20) % (margin + 1)
    lengths = lengths.at[giver].add(-shifted).at[taker].add(shifted)
    labels = jnp.searchsorted(jnp.cumsum(lengths), jnp.arange(rows * top), side="right").astype(jnp.int32)
    table = labels.reshape(top, rows).T
    table = table[jax.random.permutation(jax.random.fold_in(own, 1), rows)]
    turn = jax.random.randint(jax.random.fold_in(own, 2), (rows, 1), 0, top)
    return jnp.take_along_axis(table, (jnp.arange(top)[None, :] + turn) % top, axis=1)


def portions_of(amount, total, most, slope, full):
    portions = [(1 << 20) // math.isqrt(rank ** slope) + 1 for rank in range(1, amount + 1)]
    largest = most if full else min(most, max(-(-total // amount), total * portions[0] // sum(portions)))
    least = 1 if total - largest >= amount - 1 else 0
    counts, spare = [largest] + [least] * (amount - 1), total - largest - least * (amount - 1)
    while spare > 0:
        candidates = [i for i in range(1, amount) if counts[i] < largest] or [i for i in range(1, amount) if counts[i] < most]
        mass, remaining = sum([portions[i] for i in candidates]), spare
        for i in candidates:
            more = min(most - counts[i], max(1, remaining * portions[i] // mass), spare)
            counts[i] = counts[i] + more
            spare = spare - more
    return np.array(counts)


def bell_draw(key, extent, deviation, limit, shards=(), kind=jnp.bfloat16):
    values = jax.random.normal(key, extent, jnp.float32) * deviation
    if len(shards) > 0:
        values = shard_levels(key, extent, shards, -0.22, 0.18) * values
    return jnp.clip(values, min=-limit, max=limit).astype(kind)


def setup_inputs(seed: int = 0) -> dict:
    key_list = jax.random.split(jax.random.key(seed), 12)
    head_outputs = bell_draw(key_list[0], (TOKENS, MODEL_DIM), 1.0, 6.0, ((0, 16),))
    stream = bell_draw(key_list[1], (TOKENS, MODEL_DIM), 1.0, 6.0, ((0, 16),))
    adapter_down_factors = bell_draw(key_list[2], (MODEL_DIM, ADAPTER_COUNT * ADAPTER_RANK), MODEL_DIM ** -0.5, 0.09375, ((1, 8),))
    adapter_up_factors = bell_draw(key_list[3], (ADAPTER_COUNT * ADAPTER_RANK, MODEL_DIM), ADAPTER_RANK ** -0.5, 1.5, ((0, 8),))
    norm_gain_vector = jnp.clip(1.0 + 0.1 * jax.random.normal(key_list[4], (MODEL_DIM,), jnp.float32), 0.5, 1.5)
    router_matrix = bell_draw(key_list[5], (MODEL_DIM, E), MODEL_DIM ** -0.5, 0.09375)
    token_adapter_index = plant(skewed_ids(key_list[6], (TOKENS,), ADAPTER_COUNT, 2), jax.random.fold_in(key_list[6], 3), 0, ADAPTER_COUNT - 1).astype(jnp.int32)
    token_expert_index_keys = jax.random.split(jax.random.fold_in(key_list[7], 1), TOKENS // TOK_DEV)
    token_expert_index_turns = jax.random.permutation(jax.random.fold_in(key_list[7], 3), TOKENS // TOK_DEV)
    token_expert_index = jax.vmap(lambda own, number: deal_out(jax.random.fold_in(key_list[7], 2), own, number, TOK_DEV, E, 2, CAP, 2))(token_expert_index_keys, token_expert_index_turns).reshape((TOKENS, 2))
    gate_weight = bell_draw(key_list[8], (SLOTS, MODEL_DIM, SLOT_FF), MODEL_DIM ** -0.5, 0.09375, ((0, 16), (2, 8)))
    up_weight = bell_draw(key_list[9], (SLOTS, MODEL_DIM, SLOT_FF), MODEL_DIM ** -0.5, 0.09375, ((0, 16), (2, 8)))
    down_weight = bell_draw(key_list[10], (SLOTS, SLOT_FF, MODEL_DIM), FF ** -0.5, 0.046875, ((0, 16), (1, 8)))
    return dict(head_outputs=head_outputs, stream=stream, adapter_down_factors=adapter_down_factors, adapter_up_factors=adapter_up_factors, norm_gain_vector=norm_gain_vector, router_matrix=router_matrix, token_adapter_index=token_adapter_index, token_expert_index=token_expert_index, gate_weight=gate_weight, up_weight=up_weight, down_weight=down_weight)


EPS = 1e-05
ADAPTER_SCALE = 2.0

def reference(head_outputs, stream, adapter_down_factors, adapter_up_factors, norm_gain_vector, router_matrix, token_adapter_index, token_expert_index, gate_weight, up_weight, down_weight):
    rank_projected = jnp.dot(head_outputs, adapter_down_factors, preferred_element_type=jnp.float32)
    column_holder = jnp.arange(adapter_down_factors.shape[1], dtype=jnp.int32) // ADAPTER_RANK
    rank_projected = jnp.where(token_adapter_index[:, None] == column_holder[None, :], rank_projected, 0.0).astype(jnp.bfloat16)
    adapter_update = ADAPTER_SCALE * jnp.dot(rank_projected, adapter_up_factors, preferred_element_type=jnp.float32)
    residual_stream = stream.astype(jnp.float32) + adapter_update
    inv_norm = lax.rsqrt(lax.optimization_barrier(jnp.mean(residual_stream * residual_stream, axis=1, keepdims=True)) + EPS)
    normed = (residual_stream * inv_norm * norm_gain_vector).astype(jnp.bfloat16)
    logits = jnp.dot(normed, router_matrix, preferred_element_type=jnp.float32)
    picked = jnp.take_along_axis(logits, token_expert_index, axis=1)
    weights = 1.0 / (1.0 + jnp.exp(picked[:, ::-1] - picked))
    blocked = token_expert_index.reshape(N_BA, TOK_DEV * 2)
    expert_hits = (blocked[:, :, None] == jnp.arange(E, dtype=jnp.int32)[None, None, :]).astype(jnp.int32)
    before = jnp.cumsum(expert_hits, axis=1) - expert_hits
    position = lax.optimization_barrier(jnp.sum(before * expert_hits, axis=2))
    slot_index = (jnp.arange(N_BA, dtype=jnp.int32)[:, None] * CAP + position).reshape(-1)
    flat_experts = token_expert_index.reshape(-1)
    token_of = jnp.arange(TOKENS * 2, dtype=jnp.int32) // 2
    owner_tok = jnp.zeros((E, N_BA * CAP), jnp.int32).at[flat_experts, slot_index].set(token_of)
    halves = N_BA // E
    results = jnp.zeros((E, N_BA * CAP, normed.shape[1]), jnp.float32)
    for slot_number in range(N_BA):
        expert = slot_number // halves
        slot_rows = normed[owner_tok[expert]]
        gate_proj = jnp.dot(slot_rows, gate_weight[slot_number], preferred_element_type=jnp.float32)
        up_proj = jnp.dot(slot_rows, up_weight[slot_number], preferred_element_type=jnp.float32)
        hidden = (jax.nn.silu(gate_proj) * up_proj).astype(jnp.bfloat16)
        results = results.at[expert].add(jnp.dot(hidden, down_weight[slot_number], preferred_element_type=jnp.float32))
    expert_out = results[flat_experts, slot_index].reshape(TOKENS, 2, -1)
    mixed = residual_stream + lax.optimization_barrier(jnp.sum(weights[:, :, None] * expert_out, axis=1))
    adapter_load = lax.optimization_barrier(jnp.sum((token_adapter_index[:, None] == jnp.arange(ADAPTER_COUNT, dtype=jnp.int32)[None, :]).astype(jnp.float32), axis=0))
    return (mixed.astype(jnp.bfloat16), adapter_load)
```

```python
import jax
import jax.numpy as jnp
from jax import lax
from jax.experimental import pallas as pl
from jax.experimental.pallas import tpu as pltpu
from jax.sharding import PartitionSpec as P

MESH = pl.DeviceIdType.MESH
E = 8
RANK = 16
TOK = 128
DIM = 4096
FFD = 896
CH = 3
CR = 16
ROWS = 256
SL = 512
NT = FFD // 128
EPS = 1e-05
F32 = jnp.float32
BF16 = jnp.bfloat16


def place_of(f):
    x, core = f // 2, f % 2
    return core * 4 + (x % 2) * 2 + x // 2


def tdot(a, b):
    return lax.dot_general(a, b, (((0,), (0,)), ((), ())), preferred_element_type=F32)


def ntdot(a, b):
    return lax.dot_general(a, b, (((1,), (1,)), ((), ())), preferred_element_type=F32)


def kernel(
    head_h, stream_h, down_h, up_h, gain_ref, router_ref, idrow_ref, idcol_ref, ex_ref,
    g_h, u_h, d_h,
    out_ref, cnt_ref,
    head_v, down_v, stream_v, wgu, dv, upc, lows, low_own, stats, stat_own, lgs, lg_own, ids,
    nrm, outb, xb, hid, ysend, yrecv, yown, town, zsend, zrecv, rb, ret, mx, fsend, frecv, resid,
    load_sem, wsem, up_s, up_r, low_s, low_r, st_s, st_r, lg_s, lg_r, id_s, id_r,
    n_s, n_r, a_s, a_r, x_s, x_r, d_s, d_r, y_s, y_r, z_s, z_r, b_s, b_r, f_s, f_r,
):
    aa = lax.axis_index("aa")
    ba = lax.axis_index("ba")
    core, x = aa % 2, aa // 2
    xp, xh = x % 2, x // 2
    z, y = ba // 4, ba % 4

    def aa_at(dx, dc):
        return ((x + dx) % 4) * 2 + (core + dc) % 2

    def ba_at(d):
        return ((z + d // 4) % 4) * 4 + (y + d % 4) % 4

    def ba_from(d):
        return ((z + 4 - d // 4) % 4) * 4 + (y + 4 - d % 4) % 4

    def rcopy(src, dst, ss, rs, a, b):
        return pltpu.make_async_remote_copy(
            src_ref=src, dst_ref=dst, send_sem=ss, recv_sem=rs, device_id=(a, b),
            device_id_type=MESH,
        )

    def cols(i, width):
        return pl.ds(pl.multiple_of(i * width, width), width)

    loads = [
        pltpu.make_async_copy(head_h, head_v, load_sem.at[0]),
        pltpu.make_async_copy(down_h, down_v, load_sem.at[1]),
        pltpu.make_async_copy(stream_h.at[:, cols(aa, SL)], stream_v, load_sem.at[2]),
    ]
    for c in loads:
        c.start()

    barrier = pltpu.get_barrier_semaphore()
    for k in range(1, 8):
        pl.semaphore_signal(
            barrier, inc=1, device_id=(aa_at(k // 2, k % 2), ba), device_id_type=MESH
        )

    def greet(d, carry):
        pl.semaphore_signal(barrier, inc=1, device_id=(aa, ba_at(d)), device_id_type=MESH)
        return carry

    lax.fori_loop(1, 16, greet, 0)
    pl.semaphore_wait(barrier, 22)

    ups = []
    for k in range(1, 8):
        to = aa_at(k // 2, k % 2)
        ups.append(
            rcopy(up_h.at[:, cols(to, SL)], upc.at[k], up_s.at[k], up_r.at[k], to, ba)
        )
    for c in ups:
        c.start()
    own_up = pltpu.make_async_copy(up_h.at[:, cols(aa, SL)], upc.at[0], load_sem.at[3])
    own_up.start()

    def id_copy(d):
        return rcopy(idrow_ref, ids.at[d], id_s.at[d], id_r.at[d], aa, ba_at(d))

    def send_ids(d, carry):
        id_copy(d).start()
        return carry

    lax.fori_loop(1, 16, send_ids, 0)
    ids[0] = idrow_ref[...]

    def load_w(n, carry):
        for f in range(8):
            p = place_of(f)
            for half, w in enumerate((g_h, u_h)):
                pltpu.make_async_copy(
                    w.at[f * SL : (f + 1) * SL, cols(n, 128)],
                    wgu.at[n, p * SL : (p + 1) * SL, half * 128 : (half + 1) * 128],
                    wsem.at[0],
                ).start()
        return carry

    lax.fori_loop(0, NT, load_w, 0)
    for f in range(8):
        pltpu.make_async_copy(
            d_h.at[:, f * SL : (f + 1) * SL], dv.at[place_of(f)], wsem.at[1]
        ).start()

    for c in loads[:2]:
        c.wait()
    rank = jnp.dot(head_v[...], down_v[...], preferred_element_type=F32)
    lane = lax.broadcasted_iota(jnp.int32, (TOK, 128), 1)
    sub = lax.broadcasted_iota(jnp.int32, (TOK, 128), 0)
    idcol = idcol_ref[...]
    rank = jnp.where(idcol == aa * 8 + lane // RANK, rank, 0.0).astype(BF16)
    fold = (
        lax.broadcasted_iota(jnp.int32, (RANK, 128), 1) % RANK
        == lax.broadcasted_iota(jnp.int32, (RANK, 128), 0)
    ).astype(BF16)
    mine = ntdot(fold, rank)
    low_own[...] = mine.astype(BF16)
    lowc = []
    for k in range(1, 8):
        lowc.append(
            rcopy(low_own, lows.at[k], low_s.at[k], low_r.at[k], aa_at(k // 2, k % 2), ba)
        )
    for c in lowc:
        c.start()

    ex0, ex1 = ex_ref[0:1, :], ex_ref[1:2, :]
    e_sub = lax.broadcasted_iota(jnp.int32, (E, TOK), 0)
    hit0, hit1 = ex0 == e_sub, ex1 == e_sub
    hit = hit0 | hit1
    earlier = (sub < lane).astype(BF16)
    pos = jnp.dot(hit.astype(BF16), earlier, preferred_element_type=F32)
    pos = jnp.where(hit, pos, -1.0)
    posx = jnp.concatenate(
        [jnp.broadcast_to(pos[e : e + 1, :], (CR, TOK)) for e in range(E)], axis=0
    )
    row16 = (sub % CR).astype(F32)

    low = mine
    for k in range(1, 8):
        lowc[k - 1].wait_recv()
        low = low + lows[k].astype(F32)
    spread = tdot(low.astype(BF16), fold)

    own_up.wait()
    delta = jnp.zeros((TOK, SL), F32)
    for k in range(8):
        if k:
            ups[k - 1].wait_recv()
        src = aa_at(4 - k // 2, k % 2)
        lowk = jnp.where(idcol == src * 8 + lane // RANK, spread, 0.0).astype(BF16)
        delta = delta + jnp.dot(lowk, upc[k], preferred_element_type=F32)
    loads[2].wait()
    res = stream_v[...].astype(F32) + 2.0 * delta
    resid[...] = res
    sq = jnp.sum(res * res, axis=1, keepdims=True)
    stat_own[...] = jnp.transpose(jnp.broadcast_to(sq, (TOK, 128)))[0:8, :]
    stc = []
    for k in range(1, 8):
        stc.append(
            rcopy(stat_own, stats.at[k], st_s.at[k], st_r.at[k], aa_at(k // 2, k % 2), ba)
        )
    for c in stc:
        c.start()
    total = stat_own[...]
    for k in range(1, 8):
        stc[k - 1].wait_recv()
        total = total + stats[k]
    inv = lax.rsqrt(total[0:1, :] * (1.0 / DIM) + EPS)
    inv = jnp.transpose(jnp.broadcast_to(inv, (128, TOK)))[:, 0:1]
    own_n = (resid[...] * inv * gain_ref[:, cols(aa, SL)]).astype(BF16)
    nrm[xh] = own_n
    opp = aa_at(2, 0)
    ncopy = rcopy(nrm.at[xh], nrm.at[xh], n_s.at[0], n_r.at[0], opp, ba)
    ncopy.start()

    lg_own[...] = ntdot(router_ref[:, cols(aa, SL)], own_n)
    lgc = []
    for k in range(1, 8):
        lgc.append(
            rcopy(lg_own, lgs.at[k], lg_s.at[k], lg_r.at[k], aa_at(k // 2, k % 2), ba)
        )
    for c in lgc:
        c.start()

    grp = core * 2 + xp
    picks = [(posx == row16 + float(CR * c)).astype(BF16) for c in range(CH)]
    for c in range(CH):
        outb[c, :, cols(xh, SL)] = jnp.dot(
            picks[c], own_n, preferred_element_type=F32
        ).astype(BF16)
    ncopy.wait_recv()

    def a_copy(c, d):
        to = ba_at(d)
        return rcopy(
            outb.at[c, cols(to // 2, CR), :],
            xb.at[c, cols(ba, CR), cols(grp, 2 * SL)],
            a_s.at[c, d], a_r.at[c, d], aa, to,
        )

    for c in range(CH):
        outb[c, :, cols(1 - xh, SL)] = jnp.dot(
            picks[c], nrm[1 - xh], preferred_element_type=F32
        ).astype(BF16)

        def send_a(d, carry, c=c):
            a_copy(c, d).start()
            return carry

        lax.fori_loop(1, 16, send_a, 0)
        xb[c, cols(ba, CR), cols(grp, 2 * SL)] = outb[c, cols(ba // 2, CR), :]

    sib = aa_at(0, 1)
    place = core * 4 + xp * 2 + xh
    xc, dc1, dc2 = [], [], []
    for c in range(CH):
        sl = xb.at[c, :, cols(place, SL)]
        xc.append(
            [
                rcopy(sl, sl, x_s.at[c, 0], x_r.at[c, 0], aa_at(1, 0), ba),
                rcopy(sl, sl, x_s.at[c, 1], x_r.at[c, 1], aa_at(3, 0), ba),
            ]
        )
        g1 = xb.at[c, :, cols(grp, 2 * SL)]
        g2 = xb.at[c, :, cols(core * 2 + 1 - xp, 2 * SL)]
        dc1.append(rcopy(g1, g1, d_s.at[c, 0], d_r.at[c, 0], sib, ba))
        dc2.append(rcopy(g2, g2, d_s.at[c, 1], d_r.at[c, 1], sib, ba))

    def arrive(c):
        def wait_a(d, carry):
            a_copy(c, d).wait_recv()
            return carry

        lax.fori_loop(1, 16, wait_a, 0)
        for k in xc[c]:
            k.start()
        dc1[c].start()

    def relay(c):
        for k in xc[c]:
            k.wait_recv()
        dc2[c].start()

    def ready(c):
        dc1[c].wait_recv()
        dc2[c].wait_recv()

    def gate_up(c):
        def step(n, carry):
            gu = jnp.dot(xb[c], wgu[n], preferred_element_type=F32)
            g, u = gu[:, :128], gu[:, 128:]
            hid[:, cols(n, 128)] = (g / (1.0 + jnp.exp(-g)) * u).astype(BF16)
            return carry

        lax.fori_loop(0, NT, step, 0)

    def y_copy(c, j):
        return rcopy(ysend.at[c, j], yrecv.at[c, j], y_s.at[c, j], y_r.at[c, j], sib, ba)

    def project(c):
        def step_far(j, carry):
            ysend[c, j] = jnp.dot(
                hid[...], dv[(1 - core) * 4 + j], preferred_element_type=F32
            ).astype(BF16)
            y_copy(c, j).start()
            return carry

        lax.fori_loop(0, 4, step_far, 0)

        def step_own(j, carry):
            yown[j] = jnp.dot(hid[...], dv[core * 4 + j], preferred_element_type=F32)
            return carry

        lax.fori_loop(0, 4, step_own, 0)

    def spot(dx):
        xx = (x + dx) % 4
        return (xx % 2) * 2 + xx // 2

    zc = [
        [
            rcopy(zsend.at[c, 0], zrecv.at[c, 0], z_s.at[c, 0], z_r.at[c, 0], aa_at(1, 0), ba),
            rcopy(zsend.at[c, 1], zrecv.at[c, 1], z_s.at[c, 1], z_r.at[c, 1], aa_at(3, 0), ba),
        ]
        for c in range(CH)
    ]

    def pair_sum(c, j):
        return yown[j] + yrecv[c, j].astype(F32)

    def reduce_cores(c):
        def wait_y(j, carry):
            y_copy(c, j).wait_recv()
            return carry

        lax.fori_loop(0, 4, wait_y, 0)
        for i, dx in enumerate((1, 3)):
            zsend[c, i] = pair_sum(c, spot(dx)).astype(BF16)
            zc[c][i].start()
        rb[c, :, cols(1 - xh, SL)] = pair_sum(c, spot(2)).astype(BF16)
        town[...] = pair_sum(c, spot(0))

    def b_copy(c, d):
        to = ba_at(d)
        return rcopy(
            rb.at[c, cols(to, CR), :], ret.at[c, cols(ba, CR), :],
            b_s.at[c, d], b_r.at[c, d], aa, to,
        )

    def reduce_chips(c):
        zc[c][0].wait_recv()
        zc[c][1].wait_recv()
        rb[c, :, cols(xh, SL)] = (
            town[...] + zrecv[c, 0].astype(F32) + zrecv[c, 1].astype(F32)
        ).astype(BF16)

        def send_b(d, carry):
            b_copy(c, d).start()
            return carry

        lax.fori_loop(1, 16, send_b, 0)
        ret[c, cols(ba, CR), :] = rb[c, cols(ba, CR), :]

    def mix_weights():
        lg = lg_own[...]
        for k in range(1, 8):
            lgc[k - 1].wait_recv()
            lg = lg + lgs[k]
        l0 = jnp.sum(jnp.where(hit0, lg, 0.0), axis=0, keepdims=True)
        l1 = jnp.sum(jnp.where(hit1, lg, 0.0), axis=0, keepdims=True)
        w0 = 1.0 / (1.0 + jnp.exp(l1 - l0))
        w1 = 1.0 / (1.0 + jnp.exp(l0 - l1))
        return jnp.where(hit0, w0, 0.0) + jnp.where(hit1, w1, 0.0)

    def mix(c, wx):
        def wait_b(d, carry):
            b_copy(c, d).wait_recv()
            return carry

        lax.fori_loop(1, 16, wait_b, 0)
        w = jnp.where(posx == row16 + float(CR * c), wx, 0.0)
        hi = w.astype(BF16)
        lo = (w - hi.astype(F32)).astype(BF16)
        both = jnp.concatenate([hi, lo], axis=1)
        both = jnp.concatenate(
            [both[(s // 2) * CR : (s // 2 + 1) * CR, :] for s in range(2 * E)], axis=0
        )
        got = tdot(both, ret[c])
        got = got[:TOK, :] + got[TOK:, :]
        if c == 0:
            mx[...] = got
        else:
            mx[...] += got

    arrive(0)
    relay(0)
    arrive(1)
    ready(0)
    pltpu.make_async_copy(wgu, wgu, wsem.at[0]).wait()
    gate_up(0)
    relay(1)
    arrive(2)
    pltpu.make_async_copy(dv, dv, wsem.at[1]).wait()
    project(0)
    ready(1)
    gate_up(1)
    relay(2)
    reduce_cores(0)
    project(1)
    reduce_chips(0)
    ready(2)
    gate_up(2)
    reduce_cores(1)
    project(2)
    reduce_chips(1)
    wt = mix_weights()
    wx = jnp.concatenate(
        [jnp.broadcast_to(wt[e : e + 1, :], (CR, TOK)) for e in range(E)], axis=0
    )
    reduce_cores(2)
    mix(0, wx)
    reduce_chips(2)

    def count(d, acc):
        @pl.when(d > 0)
        def _():
            id_copy(d).wait_recv()

        row = jnp.broadcast_to(ids[d], (8, TOK))
        want = aa * 8 + lax.broadcasted_iota(jnp.int32, (8, TOK), 0)
        return acc + (row == want).astype(F32)

    tally = lax.fori_loop(0, 16, count, jnp.zeros((8, TOK), F32))
    cnt_ref[...] = jnp.broadcast_to(jnp.sum(tally, axis=1, keepdims=True), (8, TOK))

    mix(1, wx)
    mix(2, wx)
    fsend[...] = mx[:, cols(1 - xh, SL)].astype(BF16)
    fcopy = rcopy(fsend, frecv, f_s.at[0], f_r.at[0], opp, ba)
    fcopy.start()
    base = resid[...] + mx[:, cols(xh, SL)]
    fcopy.wait_recv()
    out_ref[...] = (base + frecv[...].astype(F32)).astype(BF16)

    for c in ups + lowc + stc + lgc + [ncopy, fcopy]:
        c.wait_send()

    def drain(d, carry):
        id_copy(d).wait_send()
        for c in range(CH):
            a_copy(c, d).wait_send()
            b_copy(c, d).wait_send()
        return carry

    lax.fori_loop(1, 16, drain, 0)
    for c in range(CH):
        for k in xc[c] + zc[c] + [dc1[c], dc2[c]]:
            k.wait_send()

        def drain_y(j, carry, c=c):
            y_copy(c, j).wait_send()
            return carry

        lax.fori_loop(0, 4, drain_y, 0)


def shards(
    head_outputs, stream, adapter_down_factors, adapter_up_factors, norm_gain_vector,
    router_matrix, token_adapter_index, token_expert_index, gate_weight, up_weight, down_weight,
):
    any_spec = pl.BlockSpec(memory_space=pl.ANY)
    vmem = pl.BlockSpec(memory_space=pltpu.VMEM)
    V = pltpu.VMEM
    S = pltpu.SemaphoreType.DMA
    mixed, load = pl.pallas_call(
        kernel,
        out_shape=(
            jax.ShapeDtypeStruct((TOK, SL), BF16),
            jax.ShapeDtypeStruct((8, TOK), F32),
        ),
        in_specs=[any_spec] * 4 + [vmem] * 5 + [any_spec] * 3,
        out_specs=(vmem, vmem),
        scratch_shapes=[
            V((TOK, DIM), BF16),
            V((DIM, 128), BF16),
            V((TOK, SL), BF16),
            V((NT, DIM, 256), BF16),
            V((8, FFD, SL), BF16),
            V((8, 128, SL), BF16),
            V((8, RANK, TOK), BF16),
            V((RANK, TOK), BF16),
            V((8, 8, TOK), F32),
            V((8, TOK), F32),
            V((8, E, TOK), F32),
            V((E, TOK), F32),
            V((16, 1, TOK), jnp.int32),
            V((2, TOK, SL), BF16),
            V((CH, E * CR, 2 * SL), BF16),
            V((CH, ROWS, DIM), BF16),
            V((ROWS, FFD), BF16),
            V((CH, 4, ROWS, SL), BF16),
            V((CH, 4, ROWS, SL), BF16),
            V((4, ROWS, SL), F32),
            V((ROWS, SL), F32),
            V((CH, 2, ROWS, SL), BF16),
            V((CH, 2, ROWS, SL), BF16),
            V((CH, ROWS, 2 * SL), BF16),
            V((CH, ROWS, 2 * SL), BF16),
            V((TOK, 2 * SL), F32),
            V((TOK, SL), BF16),
            V((TOK, SL), BF16),
            V((TOK, SL), F32),
            S((4,)), S((2,)),
            S((8,)), S((8,)), S((8,)), S((8,)), S((8,)), S((8,)), S((8,)), S((8,)),
            S((16,)), S((16,)),
            S((1,)), S((1,)),
            S((CH, 16)), S((CH, 16)),
            S((CH, 2)), S((CH, 2)), S((CH, 2)), S((CH, 2)),
            S((CH, 4)), S((CH, 4)),
            S((CH, 2)), S((CH, 2)),
            S((CH, 16)), S((CH, 16)),
            S((1,)), S((1,)),
        ],
        compiler_params=pltpu.CompilerParams(
            collective_id=0, has_side_effects=True, vmem_limit_bytes=66_000_000
        ),
    )(
        head_outputs, stream, adapter_down_factors, adapter_up_factors,
        norm_gain_vector.reshape(1, DIM), router_matrix.T,
        token_adapter_index.reshape(1, TOK), token_adapter_index.reshape(TOK, 1),
        token_expert_index.T, gate_weight[0], up_weight[0], down_weight[0],
    )
    return mixed, load[:, 0]


def solution(mesh):
    in_specs = (
        P("ba", None), P("ba", None), P(None, "aa"), P("aa", None), P(), P(), P("ba"),
        P("ba", None), P("ba", None, "aa"), P("ba", None, "aa"), P("ba", "aa", None),
    )
    out_specs = (P("ba", "aa"), P("aa"))
    return jax.shard_map(shards, mesh=mesh, in_specs=in_specs, out_specs=out_specs, check_vma=False)
```

```python
import jax
import jax.numpy as jnp
from jax import lax
from jax.experimental import pallas as pl
from jax.experimental.pallas import tpu as pltpu
from jax.sharding import PartitionSpec as P

MESH = pl.DeviceIdType.MESH
E = 8
RANK = 16
TOK = 128
DIM = 4096
FFD = 896
CH = 3
CR = 16
ROWS = 256
SL = 512
NT = FFD // 128
EPS = 1e-05
F32 = jnp.float32
BF16 = jnp.bfloat16


def place_of(f):
    x, core = f // 2, f % 2
    return core * 4 + (x % 2) * 2 + x // 2


def tdot(a, b):
    return lax.dot_general(a, b, (((0,), (0,)), ((), ())), preferred_element_type=F32)


def ntdot(a, b):
    return lax.dot_general(a, b, (((1,), (1,)), ((), ())), preferred_element_type=F32)


def kernel(
    head_h, stream_h, down_h, up_h, gain_ref, router_ref, idrow_ref, idcol_ref, ex_ref,
    g_h, u_h, d_h,
    out_ref, cnt_ref,
    head_v, down_v, up_v, stream_v, wgu, dv, lsend, lrecv, tsend, trecv, stats, stat_own,
    lgs, lg_own, ids, rout, routes, scl,
    nrm, outb, xb, hid, ysend, yrecv, town, zsend, zrecv, rb, ret, mx, fsend, frecv, resid,
    load_sem, wsem, l_s, l_r, t_s, t_r, st_s, st_r, lg_s, lg_r, id_s, id_r, rt_s, rt_r,
    n_s, n_r, a_s, a_r, o_s, o_r, x_s, x_r, d_s, d_r, y_s, y_r, z_s, z_r,
    b_s, b_r, q_s, q_r, f_s, f_r,
):
    aa = lax.axis_index("aa")
    ba = lax.axis_index("ba")
    core, x = aa % 2, aa // 2
    xp, xh = x % 2, x // 2
    z, y = ba // 4, ba % 4

    def aa_at(dx, dc):
        return ((x + dx) % 4) * 2 + (core + dc) % 2

    def ba_at(d):
        return ((z + d // 4) % 4) * 4 + (y + d % 4) % 4

    def ba_from(d):
        return ((z + 4 - d // 4) % 4) * 4 + (y + 4 - d % 4) % 4

    def rcopy(src, dst, ss, rs, a, b):
        return pltpu.make_async_remote_copy(
            src_ref=src, dst_ref=dst, send_sem=ss, recv_sem=rs, device_id=(a, b),
            device_id_type=MESH,
        )

    def cols(i, width):
        return pl.ds(pl.multiple_of(i * width, width), width)

    def each_peer(body):
        def step(d, carry):
            body(d)
            return carry

        lax.fori_loop(1, 16, step, 0)

    sib = aa_at(0, 1)
    opp = aa_at(2, 0)

    loads = [
        pltpu.make_async_copy(head_h, head_v, load_sem.at[0]),
        pltpu.make_async_copy(down_h, down_v, load_sem.at[1]),
        pltpu.make_async_copy(up_h, up_v, load_sem.at[2]),
        pltpu.make_async_copy(stream_h.at[:, cols(aa, SL)], stream_v, load_sem.at[3]),
    ]
    for c in loads:
        c.start()

    barrier = pltpu.get_barrier_semaphore()
    for k in range(1, 8):
        pl.semaphore_signal(
            barrier, inc=1, device_id=(aa_at(k // 2, k % 2), ba), device_id_type=MESH
        )
    each_peer(
        lambda d: pl.semaphore_signal(
            barrier, inc=1, device_id=(aa, ba_at(d)), device_id_type=MESH
        )
    )

    lane = lax.broadcasted_iota(jnp.int32, (TOK, 128), 1)
    sub = lax.broadcasted_iota(jnp.int32, (TOK, 128), 0)
    loads[0].wait()
    loads[1].wait()
    rank = jnp.dot(head_v[...], down_v[...], preferred_element_type=F32)
    rank = jnp.where(idcol_ref[...] == aa * 8 + lane // RANK, rank, 0.0).astype(BF16)
    loads[2].wait()

    def load_w(n, carry):
        for f in range(8):
            p = place_of(f)
            for half, w in enumerate((g_h, u_h)):
                pltpu.make_async_copy(
                    w.at[f * SL : (f + 1) * SL, cols(n, 128)],
                    wgu.at[n, p * SL : (p + 1) * SL, half * 128 : (half + 1) * 128],
                    wsem.at[0],
                ).start()
        return carry

    lax.fori_loop(0, NT, load_w, 0)
    for f in range(8):
        pltpu.make_async_copy(
            d_h.at[:, f * SL : (f + 1) * SL], dv.at[place_of(f)], wsem.at[1]
        ).start()

    def term(dx, dc):
        part = up_v[:, cols(aa_at(dx, dc), SL)]
        return 2.0 * jnp.dot(rank, part, preferred_element_type=F32)

    ORDER = (2, 1, 3, 0)
    for dx in ORDER:
        lsend[dx] = term(dx, 1).astype(BF16)

    pl.semaphore_wait(barrier, 22)
    lc = [rcopy(lsend.at[i], lrecv.at[i], l_s.at[i], l_r.at[i], sib, ba) for i in range(4)]
    tc = [
        rcopy(tsend.at[i], trecv.at[i], t_s.at[i], t_r.at[i], aa_at(i, 0), ba)
        for i in range(1, 4)
    ]
    for dx in ORDER:
        lc[dx].start()

    ex0, ex1 = ex_ref[0:1, :], ex_ref[1:2, :]
    e_sub = lax.broadcasted_iota(jnp.int32, (E, TOK), 0)
    hit0, hit1 = ex0 == e_sub, ex1 == e_sub
    hit = hit0 | hit1
    earlier = (sub < lane).astype(BF16)
    pos = jnp.dot(hit.astype(BF16), earlier, preferred_element_type=F32)
    pos = jnp.where(hit, pos, -1.0)
    posx = jnp.concatenate(
        [jnp.broadcast_to(pos[e : e + 1, :], (CR, TOK)) for e in range(E)], axis=0
    )
    row16 = (sub % CR).astype(F32)
    picks = [(posx == row16 + float(CR * c)).astype(BF16) for c in range(CH)]

    own_term = None
    for dx in ORDER:
        t = term(dx, 0)
        lc[dx].wait_recv()
        t = t + lrecv[dx].astype(F32)
        if dx:
            tsend[dx] = t.astype(BF16)
            tc[dx - 1].start()
        else:
            own_term = t

    def id_copy(d):
        return rcopy(idrow_ref, ids.at[d], id_s.at[d], id_r.at[d], aa, ba_at(d))

    each_peer(lambda d: id_copy(d).start())
    ids[0] = idrow_ref[...]

    loads[3].wait()
    res = stream_v[...].astype(F32) + own_term
    for c in (1, 3, 2):
        tc[c - 1].wait_recv()
        res = res + trecv[c].astype(F32)
    resid[...] = res
    gain = gain_ref[:, cols(aa, SL)]
    sq = jnp.sum(res * res, axis=1, keepdims=True)
    stat_own[...] = jnp.transpose(jnp.broadcast_to(sq, (TOK, 128)))[0:8, :]
    stc = [
        rcopy(stat_own, stats.at[k], st_s.at[k], st_r.at[k], aa_at(k // 2, k % 2), ba)
        for k in range(1, 8)
    ]
    for c in stc:
        c.start()
    own_n = (res * gain).astype(BF16)
    nrm[xh] = own_n
    ncopy = rcopy(nrm.at[xh], nrm.at[xh], n_s.at[0], n_r.at[0], opp, ba)
    ncopy.start()

    grp = core * 2 + xp

    def a_copy(c, d):
        to = ba_at(d)
        return rcopy(
            outb.at[c, cols(to // 2, CR), cols(xh, SL)],
            xb.at[c, cols(ba, CR), cols(grp * 2 + xh, SL)],
            a_s.at[c, d], a_r.at[c, d], aa, to,
        )

    def o_copy(c, d):
        to = ba_at(d)
        return rcopy(
            outb.at[c, cols(to // 2, CR), cols(1 - xh, SL)],
            xb.at[c, cols(ba, CR), cols(grp * 2 + 1 - xh, SL)],
            o_s.at[c, d], o_r.at[c, d], aa, to,
        )

    def send_rows(c, copy, half):
        outb[c, :, cols(half, SL)] = jnp.dot(
            picks[c], nrm[half], preferred_element_type=F32
        ).astype(BF16)
        each_peer(lambda d: copy(c, d).start())
        xb[c, cols(ba, CR), cols(grp * 2 + half, SL)] = outb[
            c, cols(ba // 2, CR), cols(half, SL)
        ]

    send_rows(0, a_copy, xh)
    total = stat_own[...]
    for k in range(1, 8):
        stc[k - 1].wait_recv()
        total = total + stats[k]
    inv_row = lax.rsqrt(total * (1.0 / DIM) + EPS)

    e_row = lax.broadcasted_iota(jnp.int32, (8, TOK), 0)
    for e in range(E):
        rout[e] = jnp.where(e_row == 0, jnp.broadcast_to(pos[e : e + 1, :], (8, TOK)), inv_row)

    def rt_copy(d):
        to = ba_at(d)
        return rcopy(rout.at[to // 2], routes.at[ba], rt_s.at[d], rt_r.at[d], aa, to)

    def rt_wait(d):
        src = ba_from(d)
        return rcopy(rout.at[0], routes.at[src], rt_s.at[d], rt_r.at[d], aa, src)

    each_peer(lambda d: rt_copy(d).start())
    routes[ba] = rout[ba // 2]
    send_rows(1, a_copy, xh)
    send_rows(2, a_copy, xh)

    place = core * 4 + xp * 2 + xh
    xc, dc = [], []
    for c in range(CH):
        own = xb.at[c, :, cols(place, SL)]
        far = xb.at[c, :, cols(core * 4 + xp * 2 + 1 - xh, SL)]
        near = xb.at[c, :, cols(core * 2 + 1 - xp, 2 * SL)]
        xc.append(
            [
                rcopy(own, own, x_s.at[c, 0], x_r.at[c, 0], aa_at(1, 0), ba),
                rcopy(own, own, x_s.at[c, 1], x_r.at[c, 1], aa_at(3, 0), ba),
            ]
        )
        dc.append(
            [
                rcopy(r, r, d_s.at[c, i], d_r.at[c, i], sib, ba)
                for i, r in enumerate((own, far, near))
            ]
        )

    def arrive_own(c):
        each_peer(lambda d: a_copy(c, d).wait_recv())
        for k in xc[c]:
            k.start()
        dc[c][0].start()

    def arrive_opp(c):
        each_peer(lambda d: o_copy(c, d).wait_recv())
        dc[c][1].start()

    def relay(c):
        for k in xc[c]:
            k.wait_recv()
        dc[c][2].start()

    def ready(c):
        for k in dc[c]:
            k.wait_recv()
        for s in range(16):
            r = routes[s]
            at = lax.broadcasted_iota(jnp.int32, (CR, TOK), 0).astype(F32) + float(CR * c)
            v = jnp.where(at == r[0:1, :], r[1:2, :], 0.0)
            scl[s * CR : (s + 1) * CR, :] = jnp.broadcast_to(
                jnp.sum(v, axis=1, keepdims=True), (CR, 128)
            )

    def gate_up(c):
        for n in range(NT):
            gu = jnp.dot(xb[c], wgu[n], preferred_element_type=F32)
            g, u = gu[:, :128] * scl[...], gu[:, 128:] * scl[...]
            hid[:, n * 128 : (n + 1) * 128] = (g / (1.0 + jnp.exp(-g)) * u).astype(BF16)

    zc = [
        {
            dx: rcopy(
                zsend.at[c, dx // 2], zrecv.at[c, dx // 2], z_s.at[c, dx // 2],
                z_r.at[c, dx // 2], aa_at(dx, 0), ba,
            )
            for dx in (1, 3)
        }
        for c in range(CH)
    ]
    yc = [
        [rcopy(ysend.at[c, i], yrecv.at[c, i], y_s.at[c, i], y_r.at[c, i], sib, ba) for i in range(4)]
        for c in range(CH)
    ]

    def spot(dx):
        xx = (x + dx) % 4
        return (xx % 2) * 2 + xx // 2

    def b_copy(c, d):
        to = ba_at(d)
        return rcopy(
            rb.at[c, cols(to, CR), cols(xh, SL)], ret.at[c, cols(ba, CR), cols(xh, SL)],
            b_s.at[c, d], b_r.at[c, d], aa, to,
        )

    def q_copy(c, d):
        to = ba_at(d)
        return rcopy(
            rb.at[c, cols(to, CR), cols(1 - xh, SL)], ret.at[c, cols(ba, CR), cols(1 - xh, SL)],
            q_s.at[c, d], q_r.at[c, d], aa, to,
        )

    def keep_own(c, half):
        ret[c, cols(ba, CR), cols(half, SL)] = rb[c, cols(ba, CR), cols(half, SL)]

    def project(c):
        for dx in (1, 3, 2, 0):
            ysend[c, dx] = jnp.dot(
                hid[...], dv[(1 - core) * 4 + spot(dx)], preferred_element_type=F32
            ).astype(BF16)
            yc[c][dx].start()
        for dx in (1, 3, 2, 0):
            v = jnp.dot(hid[...], dv[core * 4 + spot(dx)], preferred_element_type=F32)
            yc[c][dx].wait_recv()
            v = v + yrecv[c, dx].astype(F32)
            if dx == 0:
                town[c] = v
            elif dx == 2:
                rb[c, :, cols(1 - xh, SL)] = v.astype(BF16)
                each_peer(lambda d: q_copy(c, d).start())
                keep_own(c, 1 - xh)
            else:
                zsend[c, dx // 2] = v.astype(BF16)
                zc[c][dx].start()

    def reduce_chips(c):
        zc[c][1].wait_recv()
        zc[c][3].wait_recv()
        rb[c, :, cols(xh, SL)] = (
            town[c] + zrecv[c, 0].astype(F32) + zrecv[c, 1].astype(F32)
        ).astype(BF16)
        each_peer(lambda d: b_copy(c, d).start())
        keep_own(c, xh)

    def mix_weights():
        lg = lg_own[...]
        for k in range(1, 8):
            lgc[k - 1].wait_recv()
            lg = lg + lgs[k]
        l0 = jnp.sum(jnp.where(hit0, lg, 0.0), axis=0, keepdims=True)
        l1 = jnp.sum(jnp.where(hit1, lg, 0.0), axis=0, keepdims=True)
        w0 = 1.0 / (1.0 + jnp.exp(l1 - l0))
        w1 = 1.0 / (1.0 + jnp.exp(l0 - l1))
        return jnp.where(hit0, w0, 0.0) + jnp.where(hit1, w1, 0.0)

    def mix(c, wx, copy, half):
        each_peer(lambda d: copy(c, d).wait_recv())
        w = jnp.where(posx == row16 + float(CR * c), wx, 0.0)
        hi = w.astype(BF16)
        lo = (w - hi.astype(F32)).astype(BF16)
        both = jnp.concatenate([hi, lo], axis=1)
        both = jnp.concatenate(
            [both[(s // 2) * CR : (s // 2 + 1) * CR, :] for s in range(2 * E)], axis=0
        )
        got = tdot(both, ret[c, :, cols(half, SL)])
        got = got[:TOK, :] + got[TOK:, :]
        if c == 0:
            mx[half] = got
        else:
            mx[half] += got

    arrive_own(0)
    ncopy.wait_recv()
    for c in range(CH):
        send_rows(c, o_copy, 1 - xh)
    inv = jnp.transpose(jnp.broadcast_to(inv_row[0:1, :], (128, TOK)))[:, 0:1]
    normed = (resid[...] * inv * gain).astype(BF16)
    lg_own[...] = ntdot(router_ref[:, cols(aa, SL)], normed)
    lgc = [
        rcopy(lg_own, lgs.at[k], lg_s.at[k], lg_r.at[k], aa_at(k // 2, k % 2), ba)
        for k in range(1, 8)
    ]
    for c in lgc:
        c.start()
    arrive_own(1)
    relay(0)
    arrive_opp(0)
    arrive_own(2)
    each_peer(lambda d: rt_wait(d).wait_recv())
    ready(0)
    pltpu.make_async_copy(wgu, wgu, wsem.at[0]).wait()
    gate_up(0)
    relay(1)
    arrive_opp(1)
    pltpu.make_async_copy(dv, dv, wsem.at[1]).wait()
    project(0)
    ready(1)
    gate_up(1)
    relay(2)
    arrive_opp(2)
    reduce_chips(0)
    project(1)
    ready(2)
    gate_up(2)
    reduce_chips(1)
    wt = mix_weights()
    wx = jnp.concatenate(
        [jnp.broadcast_to(wt[e : e + 1, :], (CR, TOK)) for e in range(E)], axis=0
    )
    project(2)
    mix(0, wx, q_copy, 1 - xh)
    mix(0, wx, b_copy, xh)
    mix(1, wx, q_copy, 1 - xh)

    each_peer(lambda d: id_copy(d).wait_recv())
    want = aa * 8 + lax.broadcasted_iota(jnp.int32, (8, TOK), 0)
    tally = jnp.zeros((8, TOK), F32)
    for d in range(16):
        tally = tally + (jnp.broadcast_to(ids[d], (8, TOK)) == want).astype(F32)
    cnt_ref[...] = jnp.broadcast_to(jnp.sum(tally, axis=1, keepdims=True), (8, TOK))

    mix(2, wx, q_copy, 1 - xh)
    fsend[...] = mx[1 - xh].astype(BF16)
    fcopy = rcopy(fsend, frecv, f_s.at[0], f_r.at[0], opp, ba)
    fcopy.start()
    reduce_chips(2)
    mix(1, wx, b_copy, xh)
    mix(2, wx, b_copy, xh)
    base = resid[...] + mx[xh]
    fcopy.wait_recv()
    out_ref[...] = (base + frecv[...].astype(F32)).astype(BF16)

    for c in lc + tc + stc + lgc + [ncopy, fcopy]:
        c.wait_send()

    def drain(d):
        id_copy(d).wait_send()
        rt_copy(d).wait_send()
        for c in range(CH):
            for copy in (a_copy, o_copy, b_copy, q_copy):
                copy(c, d).wait_send()

    each_peer(drain)
    for c in range(CH):
        for k in xc[c] + list(zc[c].values()) + dc[c] + yc[c]:
            k.wait_send()


def shards(
    head_outputs, stream, adapter_down_factors, adapter_up_factors, norm_gain_vector,
    router_matrix, token_adapter_index, token_expert_index, gate_weight, up_weight, down_weight,
):
    any_spec = pl.BlockSpec(memory_space=pl.ANY)
    vmem = pl.BlockSpec(memory_space=pltpu.VMEM)
    V = pltpu.VMEM
    S = pltpu.SemaphoreType.DMA
    mixed, load = pl.pallas_call(
        kernel,
        out_shape=(
            jax.ShapeDtypeStruct((TOK, SL), BF16),
            jax.ShapeDtypeStruct((8, TOK), F32),
        ),
        in_specs=[any_spec] * 4 + [vmem] * 5 + [any_spec] * 3,
        out_specs=(vmem, vmem),
        scratch_shapes=[
            V((TOK, DIM), BF16),
            V((DIM, 128), BF16),
            V((128, DIM), BF16),
            V((TOK, SL), BF16),
            V((NT, DIM, 256), BF16),
            V((8, FFD, SL), BF16),
            V((4, TOK, SL), BF16),
            V((4, TOK, SL), BF16),
            V((4, TOK, SL), BF16),
            V((4, TOK, SL), BF16),
            V((8, 8, TOK), F32),
            V((8, TOK), F32),
            V((8, E, TOK), F32),
            V((E, TOK), F32),
            V((16, 1, TOK), jnp.int32),
            V((E, 8, TOK), F32),
            V((16, 8, TOK), F32),
            V((ROWS, 128), F32),
            V((2, TOK, SL), BF16),
            V((CH, E * CR, 2 * SL), BF16),
            V((CH, ROWS, DIM), BF16),
            V((ROWS, FFD), BF16),
            V((CH, 4, ROWS, SL), BF16),
            V((CH, 4, ROWS, SL), BF16),
            V((CH, ROWS, SL), F32),
            V((CH, 2, ROWS, SL), BF16),
            V((CH, 2, ROWS, SL), BF16),
            V((CH, ROWS, 2 * SL), BF16),
            V((CH, ROWS, 2 * SL), BF16),
            V((2, TOK, SL), F32),
            V((TOK, SL), BF16),
            V((TOK, SL), BF16),
            V((TOK, SL), F32),
            S((4,)), S((2,)),
            S((4,)), S((4,)), S((4,)), S((4,)), S((8,)), S((8,)), S((8,)), S((8,)),
            S((16,)), S((16,)), S((16,)), S((16,)),
            S((1,)), S((1,)),
            S((CH, 16)), S((CH, 16)), S((CH, 16)), S((CH, 16)),
            S((CH, 2)), S((CH, 2)), S((CH, 3)), S((CH, 3)),
            S((CH, 4)), S((CH, 4)),
            S((CH, 2)), S((CH, 2)),
            S((CH, 16)), S((CH, 16)), S((CH, 16)), S((CH, 16)),
            S((1,)), S((1,)),
        ],
        compiler_params=pltpu.CompilerParams(
            collective_id=0, has_side_effects=True, vmem_limit_bytes=66_000_000
        ),
    )(
        head_outputs, stream, adapter_down_factors, adapter_up_factors,
        norm_gain_vector.reshape(1, DIM), router_matrix.T,
        token_adapter_index.reshape(1, TOK), token_adapter_index.reshape(TOK, 1),
        token_expert_index.T, gate_weight[0], up_weight[0], down_weight[0],
    )
    return mixed, load[:, 0]


def solution(mesh):
    in_specs = (
        P("ba", None), P("ba", None), P(None, "aa"), P("aa", None), P(), P(), P("ba"),
        P("ba", None), P("ba", None, "aa"), P("ba", None, "aa"), P("ba", "aa", None),
    )
    out_specs = (P("ba", "aa"), P("aa"))
    return jax.shard_map(shards, mesh=mesh, in_specs=in_specs, out_specs=out_specs, check_vma=False)
```

```python
import jax
import jax.numpy as jnp
from jax import lax
from jax.experimental import pallas as pl
from jax.experimental.pallas import tpu as pltpu
from jax.sharding import PartitionSpec as P

MESH = pl.DeviceIdType.MESH
E = 8
RANK = 16
TOK = 128
DIM = 4096
FFD = 896
CH = 3
CR = 16
ROWS = 256
SL = 512
NT = FFD // 128
EPS = 1e-05
F32 = jnp.float32
BF16 = jnp.bfloat16


def place_of(f):
    x, core = f // 2, f % 2
    return (x % 2) * 4 + core * 2 + x // 2


def tdot(a, b):
    return lax.dot_general(a, b, (((0,), (0,)), ((), ())), preferred_element_type=F32)


def ntdot(a, b):
    return lax.dot_general(a, b, (((1,), (1,)), ((), ())), preferred_element_type=F32)


def kernel(
    head_h, stream_h, down_h, up_h, gain_h, router_h, idrow_h, ex_h,
    g_h, u_h, d_h,
    out_ref, cnt_ref,
    head_v, down_v, up_v, stream_v, gain_ref, router_ref, idrow_ref, ex_ref, wgu, dv, lsend, lrecv, tsend, trecv, stats, stat_own,
    lgs, lg_own, ids, rout, routes, scl,
    nrm, outb, xb, hid, ysend, yrecv, near, town, zsend, zrecv, rb, ret, mx, fsend, frecv, resid, acc,
    load_sem, wsem, l_s, l_r, t_s, t_r, st_s, st_r, lg_s, lg_r, id_s, id_r, rt_s, rt_r,
    n_s, n_r, a_s, a_r, x_s, x_r, d_s, d_r, y_s, y_r, z_s, z_r,
    b_s, b_r, f_s, f_r,
):
    aa = lax.axis_index("aa")
    ba = lax.axis_index("ba")
    rem, div = lax.rem, lax.div
    core, x = rem(aa, 2), div(aa, 2)
    xp, xh = rem(x, 2), div(x, 2)
    z, y = div(ba, 4), rem(ba, 4)

    def aa_at(dx, dc):
        return rem(x + dx, 4) * 2 + rem(core + dc, 2)

    def ba_at(d):
        return rem(z + div(d, 4), 4) * 4 + rem(y + rem(d, 4), 4)

    def take(ref, sem):
        pltpu.make_async_copy(ref, ref, sem).wait()

    def rcopy(src, dst, ss, rs, a, b):
        return pltpu.make_async_remote_copy(
            src_ref=src, dst_ref=dst, send_sem=ss, recv_sem=rs, device_id=(a, b),
            device_id_type=MESH,
        )

    def cols(i, width):
        return pl.ds(pl.multiple_of(i * width, width), width)

    def each_peer(body):
        def step(d, carry):
            body(d)
            return carry

        lax.fori_loop(1, 16, step, 0)

    sib = aa_at(0, 1)
    opp = aa_at(2, 0)

    loads = [
        pltpu.make_async_copy(head_h, head_v, load_sem.at[0]),
        pltpu.make_async_copy(down_h, down_v, load_sem.at[1]),
        pltpu.make_async_copy(up_h, up_v, load_sem.at[2]),
        pltpu.make_async_copy(idrow_h, idrow_ref, load_sem.at[4]),
        pltpu.make_async_copy(stream_h.at[:, cols(aa, SL)], stream_v, load_sem.at[3]),
        pltpu.make_async_copy(gain_h.at[:, cols(aa, SL)], gain_ref, load_sem.at[5]),
        pltpu.make_async_copy(router_h.at[:, cols(aa, SL)], router_ref, load_sem.at[6]),
        pltpu.make_async_copy(ex_h, ex_ref, load_sem.at[7]),
    ]
    for c in loads:
        c.start()

    barrier = pltpu.get_barrier_semaphore()
    for k in range(1, 8):
        pl.semaphore_signal(
            barrier, inc=1, device_id=(aa_at(k // 2, k % 2), ba), device_id_type=MESH
        )
    each_peer(
        lambda d: pl.semaphore_signal(
            barrier, inc=1, device_id=(aa, ba_at(d)), device_id_type=MESH
        )
    )

    lane = lax.broadcasted_iota(jnp.int32, (TOK, 128), 1)
    sub = lax.broadcasted_iota(jnp.int32, (TOK, 128), 0)
    loads[0].wait()
    loads[1].wait()
    loads[3].wait()
    rank = jnp.dot(head_v[...], down_v[...], preferred_element_type=F32)
    idcol = jnp.transpose(jnp.broadcast_to(idrow_ref[...].astype(F32), (128, TOK)))
    rank = jnp.where(idcol == (aa * 8 + lane // RANK).astype(F32), rank, 0.0).astype(BF16)
    loads[2].wait()

    def load_w(n, carry):
        for f in range(8):
            p = place_of(f)
            for half, w in enumerate((g_h, u_h)):
                pltpu.make_async_copy(
                    w.at[f * SL : (f + 1) * SL, cols(n, 128)],
                    wgu.at[n, p * SL : (p + 1) * SL, half * 128 : (half + 1) * 128],
                    wsem.at[0],
                ).start()
        return carry

    lax.fori_loop(0, NT, load_w, 0)
    for f in range(8):
        pltpu.make_async_copy(
            d_h.at[:, f * SL : (f + 1) * SL],
            dv.at[place_of(f) // 2, :, (place_of(f) % 2) * SL : (place_of(f) % 2 + 1) * SL],
            wsem.at[1],
        ).start()

    def term(dx, dc):
        part = up_v[:, cols(aa_at(dx, dc), SL)]
        return 2.0 * jnp.dot(rank, part, preferred_element_type=F32)

    ORDER = (2, 1, 3, 0)
    for dx in ORDER:
        lsend[dx] = term(dx, 1).astype(BF16)

    pl.semaphore_wait(barrier, 22)
    lc = [rcopy(lsend.at[i], lrecv.at[i], l_s.at[i], l_r.at[i], sib, ba) for i in range(4)]
    tc = [
        rcopy(tsend.at[i], trecv.at[i], t_s.at[i], t_r.at[i], aa_at(i, 0), ba)
        for i in range(1, 4)
    ]
    for dx in ORDER:
        lc[dx].start()

    loads[7].wait()
    ex0, ex1 = ex_ref[0:1, :], ex_ref[1:2, :]
    e_sub = lax.broadcasted_iota(jnp.int32, (E, TOK), 0)
    hit0, hit1 = ex0 == e_sub, ex1 == e_sub
    hit = hit0 | hit1
    earlier = (sub < lane).astype(BF16)
    pos = jnp.dot(hit.astype(BF16), earlier, preferred_element_type=F32)
    pos = jnp.where(hit, pos, -1.0)
    posx = jnp.concatenate(
        [jnp.broadcast_to(pos[e : e + 1, :], (CR, TOK)) for e in range(E)], axis=0
    )
    row16 = (sub % CR).astype(F32)
    picks = [(posx == row16 + float(CR * c)).astype(BF16) for c in range(CH)]

    own_term = None
    for dx in ORDER:
        t = term(dx, 0)
        lc[dx].wait_recv()
        t = t + lrecv[dx].astype(F32)
        if dx:
            tsend[dx] = t.astype(BF16)
            tc[dx - 1].start()
        else:
            own_term = t

    def id_copy(d):
        return rcopy(idrow_ref, ids.at[d], id_s.at[0], id_r.at[0], aa, ba_at(d))

    each_peer(lambda d: id_copy(d).start())
    ids[0] = idrow_ref[...]

    for c in loads[4:7]:
        c.wait()
    res = stream_v[...].astype(F32) + own_term
    for c in (1, 3, 2):
        tc[c - 1].wait_recv()
        res = res + trecv[c].astype(F32)
    resid[...] = res
    gain = gain_ref[...]
    sq = jnp.sum(res * res, axis=1, keepdims=True)
    stat_own[...] = jnp.transpose(jnp.broadcast_to(sq, (TOK, 128)))[0:8, :]
    stc = [
        rcopy(stat_own, stats.at[k], st_s.at[0], st_r.at[0], aa_at(k // 2, k % 2), ba)
        for k in range(1, 8)
    ]
    for c in stc:
        c.start()
    own_n = (res * gain).astype(BF16)
    nrm[xh] = own_n
    ncopy = rcopy(nrm.at[xh], nrm.at[xh], n_s.at[0], n_r.at[0], opp, ba)
    ncopy.start()

    grp = xp * 2 + core

    def a_copy(c, d):
        to = ba_at(d)
        return rcopy(
            outb.at[c, cols(div(to, 2), CR), cols(xh, SL)],
            xb.at[c, cols(ba, CR), cols(grp * 2 + xh, SL)],
            a_s.at[c, 0], a_r.at[c, 0], aa, to,
        )

    def o_copy(c, d):
        to = ba_at(d)
        return rcopy(
            outb.at[c, cols(div(to, 2), CR), cols(1 - xh, SL)],
            xb.at[c, cols(ba, CR), cols(grp * 2 + 1 - xh, SL)],
            a_s.at[c, 1], a_r.at[c, 1], aa, to,
        )

    def w_copy(c, d):
        to = ba_at(d)
        return rcopy(
            outb.at[c, cols(div(to, 2), CR), :],
            xb.at[c, cols(ba, CR), cols(grp, 2 * SL)],
            a_s.at[c, 0], a_r.at[c, 0], aa, to,
        )

    def fill(c, half):
        outb[c, :, cols(half, SL)] = jnp.dot(
            picks[c], nrm[half], preferred_element_type=F32
        ).astype(BF16)

    def send_rows(copy, c, at, width):
        each_peer(lambda d: copy(c, d).start())
        xb[c, cols(ba, CR), cols(grp * (2 * SL // width) + at, width)] = outb[
            c, cols(div(ba, 2), CR), cols(at, width)
        ]

    fill(0, xh)
    send_rows(a_copy, 0, xh, SL)
    total = stat_own[...]
    take(stats.at[pl.ds(1, 7)], st_r.at[0])
    for k in range(1, 8):
        total = total + stats[k]
    inv_row = lax.rsqrt(total * (1.0 / DIM) + EPS)

    e_row = lax.broadcasted_iota(jnp.int32, (8, TOK), 0)
    for e in range(E):
        rout[e] = jnp.where(e_row == 0, jnp.broadcast_to(pos[e : e + 1, :], (8, TOK)), inv_row)

    def rt_copy(d):
        to = ba_at(d)
        return rcopy(rout.at[div(to, 2)], routes.at[ba], rt_s.at[0], rt_r.at[0], aa, to)

    each_peer(lambda d: rt_copy(d).start())
    routes[ba] = rout[div(ba, 2)]
    fill(1, xh)
    send_rows(a_copy, 1, xh, SL)
    fill(2, xh)

    place = grp * 2 + xh
    xc, dc = [], []
    for c in range(CH):
        own = xb.at[c, :, cols(place, SL)]
        far = xb.at[c, :, cols(grp * 2 + 1 - xh, SL)]
        mine = xb.at[c, :, cols(grp, 2 * SL)]
        side = xb.at[c, :, cols((1 - xp) * 2 + core, 2 * SL)]
        xc.append(
            [
                rcopy(own, own, x_s.at[c, 0], x_r.at[c, 0], aa_at(1, 0), ba),
                rcopy(own, own, x_s.at[c, 1], x_r.at[c, 1], aa_at(3, 0), ba),
            ]
        )
        dc.append(
            [
                rcopy(r, r, d_s.at[c, i], d_r.at[c, i], sib, ba)
                for i, r in enumerate((own, far, side) if c < 2 else (mine, side))
            ]
        )

    half_ret = ret.at[0, pl.ds(0, ROWS - CR), pl.ds(0, SL)]
    full_ret = ret.at[0, pl.ds(0, ROWS - CR), :]
    half_rows = xb.at[0, pl.ds(0, ROWS - CR), pl.ds(0, SL)]
    full_rows = xb.at[0, pl.ds(0, ROWS - CR), pl.ds(0, 2 * SL)]

    def cross(c):
        for k in xc[c]:
            k.start()

    def arrive_own(c):
        take(half_rows, a_r.at[c, 0])
        if c == 0:
            cross(c)
        dc[c][0].start()

    def arrive_opp(c):
        take(half_rows, a_r.at[c, 1])
        dc[c][1].start()

    def arrive(c):
        take(full_rows, a_r.at[c, 0])
        for k in xc[c]:
            k.start()
        dc[c][0].start()

    def relay(c):
        for k in xc[c]:
            k.wait_recv()
        dc[c][-1].start()

    def scales(c):
        for s in range(16):
            r = routes[s]
            at = lax.broadcasted_iota(jnp.int32, (CR, TOK), 0).astype(F32) + float(CR * c)
            v = jnp.where(at == r[0:1, :], r[1:2, :], 0.0)
            scl[s * CR : (s + 1) * CR, :] = jnp.broadcast_to(
                jnp.sum(v, axis=1, keepdims=True), (CR, 128)
            )

    def activate(n, gu):
        g, u = gu[:, :128] * scl[...], gu[:, 128:] * scl[...]
        hid[:, n * 128 : (n + 1) * 128] = (g / (1.0 + jnp.exp(-g)) * u).astype(BF16)

    def part(n, which):
        return jnp.dot(
            xb[0, :, cols(which, 2048)], wgu[n, cols(which, 2048), :], preferred_element_type=F32
        )

    def gate_up(c):
        for n in range(NT):
            if c == 2 and n == 4:
                reduce_chips(0)
            activate(n, jnp.dot(xb[c], wgu[n], preferred_element_type=F32))

    def z_copy(c, dx):
        half = div(rem(x + dx, 4), 2)
        return rcopy(
            zsend.at[c, :, cols(half, SL)], zrecv.at[c, dx // 2], z_s.at[c, dx // 2],
            z_r.at[c, dx // 2], aa_at(dx, 0), ba,
        )

    zc = [{dx: z_copy(c, dx) for dx in (1, 3)} for c in range(CH)]
    yc = [
        [rcopy(ysend.at[c, i], yrecv.at[c, i], y_s.at[c, i], y_r.at[c, i], sib, ba) for i in range(2)]
        for c in range(CH)
    ]

    def b_copy(c, d):
        to = ba_at(d)
        return rcopy(
            rb.at[c, cols(to, CR), cols(xh, SL)], ret.at[c, cols(ba, CR), cols(xh, SL)],
            b_s.at[c, 0], b_r.at[c, 0], aa, to,
        )

    def q_copy(c, d):
        to = ba_at(d)
        return rcopy(
            rb.at[c, cols(to, CR), cols(1 - xh, SL)], ret.at[c, cols(ba, CR), cols(1 - xh, SL)],
            b_s.at[c, 1], b_r.at[c, 1], aa, to,
        )

    def v_copy(c, d):
        to = ba_at(d)
        return rcopy(
            rb.at[c, cols(to, CR), :], ret.at[c, cols(ba, CR), :],
            b_s.at[c, 0], b_r.at[c, 0], aa, to,
        )

    def down(group):
        return jnp.dot(hid[...], dv[group], preferred_element_type=F32)

    def project(c, before, after):
        for i, g in enumerate((1 - xp, xp)):
            ysend[c, i] = down(g * 2 + 1 - core).astype(BF16)
            yc[c][i].start()
        near[...] = down((1 - xp) * 2 + core)
        before()
        town[c] = down(xp * 2 + core)
        yc[c][0].wait_recv()
        zsend[c] = (near[...] + yrecv[c, 0].astype(F32)).astype(BF16)
        zc[c][1].start()
        zc[c][3].start()
        after()
        yc[c][1].wait_recv()
        v = town[c] + yrecv[c, 1].astype(F32)
        town[c] = v
        rb[c] = v.astype(BF16)
        if c:
            each_peer(lambda d: q_copy(c, d).start())
            ret[c, cols(ba, CR), cols(1 - xh, SL)] = rb[c, cols(ba, CR), cols(1 - xh, SL)]

    def reduce_chips(c):
        zc[c][1].wait_recv()
        zc[c][3].wait_recv()
        rb[c, :, cols(xh, SL)] = (
            town[c, :, cols(xh, SL)] + zrecv[c, 0].astype(F32) + zrecv[c, 1].astype(F32)
        ).astype(BF16)
        if c:
            each_peer(lambda d: b_copy(c, d).start())
            ret[c, cols(ba, CR), cols(xh, SL)] = rb[c, cols(ba, CR), cols(xh, SL)]
        else:
            each_peer(lambda d: v_copy(c, d).start())
            ret[c, cols(ba, CR), :] = rb[c, cols(ba, CR), :]

    def mix_weights():
        lg = lg_own[...]
        take(lgs.at[pl.ds(1, 7)], lg_r.at[0])
        for k in range(1, 8):
            lg = lg + lgs[k]
        l0 = jnp.sum(jnp.where(hit0, lg, 0.0), axis=0, keepdims=True)
        l1 = jnp.sum(jnp.where(hit1, lg, 0.0), axis=0, keepdims=True)
        w0 = 1.0 / (1.0 + jnp.exp(l1 - l0))
        w1 = 1.0 / (1.0 + jnp.exp(l0 - l1))
        return jnp.where(hit0, w0, 0.0) + jnp.where(hit1, w1, 0.0)

    def spread_weights(c, wx):
        w = jnp.where(posx == row16 + float(CR * c), wx, 0.0)
        hi = w.astype(BF16)
        lo = (w - hi.astype(F32)).astype(BF16)
        both = jnp.concatenate([hi, lo], axis=1)
        return jnp.concatenate(
            [both[(s // 2) * CR : (s // 2 + 1) * CR, :] for s in range(2 * E)], axis=0
        )

    def mix(c, wx, half):
        got = tdot(spread_weights(c, wx), ret[c, :, cols(half, SL)])
        got = got[:TOK, :] + got[TOK:, :]
        if c == 0:
            mx[half] = got
        else:
            mx[half] += got

    arrive_own(0)
    ncopy.wait_recv()
    fill(0, 1 - xh)
    send_rows(o_copy, 0, 1 - xh, SL)
    fill(1, 1 - xh)
    send_rows(o_copy, 1, 1 - xh, SL)
    fill(2, 1 - xh)
    inv = jnp.transpose(jnp.broadcast_to(inv_row[0:1, :], (128, TOK)))[:, 0:1]
    normed = (resid[...] * inv * gain).astype(BF16)
    lg_own[...] = ntdot(router_ref[...], normed)
    lgc = [
        rcopy(lg_own, lgs.at[k], lg_s.at[0], lg_r.at[0], aa_at(k // 2, k % 2), ba)
        for k in range(1, 8)
    ]
    for c in lgc:
        c.start()
    arrive_own(1)
    take(routes.at[pl.ds(0, 15)], rt_r.at[0])
    scales(0)
    send_rows(w_copy, 2, 0, 2 * SL)
    arrive_opp(0)
    cross(1)
    dc[0][0].wait_recv()
    dc[0][1].wait_recv()
    pltpu.make_async_copy(wgu, wgu, wsem.at[0]).wait()
    for n in range(5):
        acc[n] = part(n, xp)
    relay(0)
    for n in range(5, NT):
        acc[n] = part(n, xp)
    arrive_opp(1)
    dc[0][2].wait_recv()
    for n in range(NT):
        activate(n, acc[n] + part(n, 1 - xp))
    pltpu.make_async_copy(dv, dv, wsem.at[1]).wait()
    project(0, lambda: (arrive(2), relay(1)), lambda: None)
    scales(1)
    for k in dc[1]:
        k.wait_recv()
    gate_up(1)
    project(1, lambda: None, lambda: relay(2))
    scales(2)
    for k in dc[2][:2]:
        k.wait_recv()
    gate_up(2)
    wt = mix_weights()
    wx = jnp.concatenate(
        [jnp.broadcast_to(wt[e : e + 1, :], (CR, TOK)) for e in range(E)], axis=0
    )
    project(2, lambda: None, lambda: None)
    reduce_chips(1)
    take(full_ret, b_r.at[0, 0])
    mix(0, wx, 1 - xh)
    mix(0, wx, xh)

    take(ids.at[pl.ds(1, 15)], id_r.at[0])
    want = aa * 8 + lax.broadcasted_iota(jnp.int32, (8, TOK), 0)
    tally = jnp.zeros((8, TOK), F32)
    for d in range(16):
        tally = tally + (jnp.broadcast_to(ids[d], (8, TOK)) == want).astype(F32)
    cnt_ref[...] = jnp.broadcast_to(jnp.sum(tally, axis=1, keepdims=True), (8, TOK))

    take(half_ret, b_r.at[1, 1])
    mix(1, wx, 1 - xh)
    reduce_chips(2)
    take(half_ret, b_r.at[2, 1])
    mix(2, wx, 1 - xh)
    fsend[...] = mx[1 - xh].astype(BF16)
    fcopy = rcopy(fsend, frecv, f_s.at[0], f_r.at[0], opp, ba)
    fcopy.start()
    take(half_ret, b_r.at[1, 0])
    mix(1, wx, xh)
    take(half_ret, b_r.at[2, 0])
    mix(2, wx, xh)
    base = resid[...] + mx[xh]
    fcopy.wait_recv()
    out_ref[...] = (base + frecv[...].astype(F32)).astype(BF16)

    for c in lc + tc + [ncopy, fcopy]:
        c.wait_send()
    take(ids.at[pl.ds(1, 15)], id_s.at[0])
    take(stats.at[pl.ds(1, 7)], st_s.at[0])
    take(lgs.at[pl.ds(1, 7)], lg_s.at[0])
    take(routes.at[pl.ds(0, 15)], rt_s.at[0])
    for c in range(2):
        take(half_rows, a_s.at[c, 0])
        take(half_rows, a_s.at[c, 1])
    take(full_rows, a_s.at[2, 0])
    take(full_ret, b_s.at[0, 0])
    for c in (1, 2):
        take(half_ret, b_s.at[c, 0])
        take(half_ret, b_s.at[c, 1])
    for c in range(CH):
        for k in xc[c] + list(zc[c].values()) + dc[c] + yc[c]:
            k.wait_send()


def shards(
    head_outputs, stream, adapter_down_factors, adapter_up_factors, norm_gain_vector,
    router_matrix, token_adapter_index, token_expert_index, gate_weight, up_weight, down_weight,
):
    hbm = pl.BlockSpec(memory_space=pltpu.HBM)
    vmem = pl.BlockSpec(memory_space=pltpu.VMEM)
    V = pltpu.VMEM
    S = pltpu.SemaphoreType.DMA
    mixed, load = pl.pallas_call(
        kernel,
        out_shape=(
            jax.ShapeDtypeStruct((TOK, SL), BF16),
            jax.ShapeDtypeStruct((8, TOK), F32),
        ),
        in_specs=[hbm] * 11,
        out_specs=(vmem, vmem),
        scratch_shapes=[
            V((TOK, DIM), BF16),
            V((DIM, 128), BF16),
            V((128, DIM), BF16),
            V((TOK, SL), BF16),
            V((1, SL), F32),
            V((E, SL), BF16),
            V((1, TOK), jnp.int32),
            V((2, TOK), jnp.int32),
            V((NT, DIM, 256), BF16),
            V((4, FFD, 2 * SL), BF16),
            V((4, TOK, SL), BF16),
            V((4, TOK, SL), BF16),
            V((4, TOK, SL), BF16),
            V((4, TOK, SL), BF16),
            V((8, 8, TOK), F32),
            V((8, TOK), F32),
            V((8, E, TOK), F32),
            V((E, TOK), F32),
            V((16, 1, TOK), jnp.int32),
            V((E, 8, TOK), F32),
            V((16, 8, TOK), F32),
            V((ROWS, 128), F32),
            V((2, TOK, SL), BF16),
            V((CH, E * CR, 2 * SL), BF16),
            V((CH, ROWS, DIM), BF16),
            V((ROWS, FFD), BF16),
            V((CH, 2, ROWS, 2 * SL), BF16),
            V((CH, 2, ROWS, 2 * SL), BF16),
            V((ROWS, 2 * SL), F32),
            V((CH, ROWS, 2 * SL), F32),
            V((CH, ROWS, 2 * SL), BF16),
            V((CH, 2, ROWS, SL), BF16),
            V((CH, ROWS, 2 * SL), BF16),
            V((CH, ROWS, 2 * SL), BF16),
            V((2, TOK, SL), F32),
            V((TOK, SL), BF16),
            V((TOK, SL), BF16),
            V((TOK, SL), F32),
            V((NT, ROWS, 256), F32),
            S((8,)), S((2,)),
            S((4,)), S((4,)), S((4,)), S((4,)), S((1,)), S((1,)), S((1,)), S((1,)),
            S((1,)), S((1,)), S((1,)), S((1,)),
            S((1,)), S((1,)),
            S((CH, 2)), S((CH, 2)),
            S((CH, 2)), S((CH, 2)), S((CH, 3)), S((CH, 3)),
            S((CH, 2)), S((CH, 2)),
            S((CH, 2)), S((CH, 2)),
            S((CH, 2)), S((CH, 2)),
            S((1,)), S((1,)),
        ],
        compiler_params=pltpu.CompilerParams(
            collective_id=0, has_side_effects=True, vmem_limit_bytes=56_000_000
        ),
    )(*[pltpu.with_memory_space_constraint(a, pltpu.HBM) for a in (
        head_outputs, stream, adapter_down_factors, adapter_up_factors,
        norm_gain_vector.reshape(1, DIM), router_matrix.T,
        token_adapter_index.reshape(1, TOK),
        token_expert_index.T, gate_weight[0], up_weight[0], down_weight[0],
    )])
    return mixed, load[:, 0]


def solution(mesh):
    in_specs = (
        P("ba", None), P("ba", None), P(None, "aa"), P("aa", None), P(), P(), P("ba"),
        P("ba", None), P("ba", None, "aa"), P("ba", None, "aa"), P("ba", "aa", None),
    )
    out_specs = (P("ba", "aa"), P("aa"))
    return jax.shard_map(shards, mesh=mesh, in_specs=in_specs, out_specs=out_specs, check_vma=False)
```

```python
import jax
import jax.numpy as jnp
from jax import lax
from jax.experimental import pallas as pl
from jax.experimental.pallas import tpu as pltpu
from jax.sharding import PartitionSpec as P

MESH = pl.DeviceIdType.MESH
E = 8
RANK = 16
TOK = 128
DIM = 4096
FFD = 896
CH = 3
CR = 16
ROWS = 256
SL = 512
HS = SL // 2
NT = FFD // 128
EPS = 1e-05
F32 = jnp.float32
BF16 = jnp.bfloat16


def place_of(f):
    x, core = f // 2, f % 2
    return (x % 2) * 4 + core * 2 + x // 2


def tdot(a, b):
    return lax.dot_general(a, b, (((0,), (0,)), ((), ())), preferred_element_type=F32)


def ntdot(a, b):
    return lax.dot_general(a, b, (((1,), (1,)), ((), ())), preferred_element_type=F32)


def kernel(
    head_h, stream_h, down_h, up_h, gain_h, router_h, idrow_h, ex_h,
    g_h, u_h, d_h,
    out_ref, cnt_ref,
    head_v, down_v, up_v, stream_v, gain_ref, router_ref, idrow_ref, ex_ref, wgu, dv, lsend, lrecv, tsend, trecv, stats, stat_own,
    lgs, lg_own, ids, rout, routes, scl,
    nrm, outb, xb, hid, ysend, yrecv, near, town, zsend, zrecv, rb, ret, mx, fsend, frecv, resid, acc,
    load_sem, wsem, l_s, l_r, t_s, t_r, st_s, st_r, lg_s, lg_r, id_s, id_r, rt_s, rt_r,
    n_s, n_r, a_s, a_r, x_s, x_r, d_s, d_r, y_s, y_r, z_s, z_r,
    b_s, b_r, f_s, f_r,
):
    aa = lax.axis_index("aa")
    ba = lax.axis_index("ba")
    rem, div = lax.rem, lax.div
    core, x = rem(aa, 2), div(aa, 2)
    xp, xh = rem(x, 2), div(x, 2)
    z, y = div(ba, 4), rem(ba, 4)

    def aa_at(dx, dc):
        return rem(x + dx, 4) * 2 + rem(core + dc, 2)

    peers = [rem(z + d // 4, 4) * 4 + rem(y + d % 4, 4) for d in range(16)]

    def ba_at(d):
        return peers[d]

    def take(ref, sem):
        pltpu.make_async_copy(ref, ref, sem).wait()

    def rcopy(src, dst, ss, rs, a, b):
        return pltpu.make_async_remote_copy(
            src_ref=src, dst_ref=dst, send_sem=ss, recv_sem=rs, device_id=(a, b),
            device_id_type=MESH,
        )

    def cols(i, width):
        return pl.ds(pl.multiple_of(i * width, width), width)

    def each_peer(body):
        for d in range(1, 16):
            body(d)

    sib = aa_at(0, 1)
    opp = aa_at(2, 0)

    loads = [
        pltpu.make_async_copy(head_h, head_v, load_sem.at[0]),
        pltpu.make_async_copy(down_h, down_v, load_sem.at[1]),
        pltpu.make_async_copy(up_h, up_v, load_sem.at[2]),
        pltpu.make_async_copy(idrow_h, idrow_ref, load_sem.at[4]),
        pltpu.make_async_copy(stream_h.at[:, cols(aa, SL)], stream_v, load_sem.at[3]),
        pltpu.make_async_copy(gain_h.at[:, cols(aa, SL)], gain_ref, load_sem.at[5]),
        pltpu.make_async_copy(router_h.at[:, cols(aa, SL)], router_ref, load_sem.at[6]),
        pltpu.make_async_copy(ex_h, ex_ref, load_sem.at[7]),
    ]
    for c in loads:
        c.start()

    barrier = pltpu.get_barrier_semaphore()
    for k in range(1, 8):
        pl.semaphore_signal(
            barrier, inc=1, device_id=(aa_at(k // 2, k % 2), ba), device_id_type=MESH
        )
    each_peer(
        lambda d: pl.semaphore_signal(
            barrier, inc=1, device_id=(aa, ba_at(d)), device_id_type=MESH
        )
    )

    lane = lax.broadcasted_iota(jnp.int32, (TOK, 128), 1)
    sub = lax.broadcasted_iota(jnp.int32, (TOK, 128), 0)
    loads[0].wait()
    loads[1].wait()
    loads[3].wait()
    rank = jnp.dot(head_v[...], down_v[...], preferred_element_type=F32)
    idcol = jnp.transpose(jnp.broadcast_to(idrow_ref[...].astype(F32), (128, TOK)))
    rank = jnp.where(idcol == (aa * 8 + lane // RANK).astype(F32), rank, 0.0).astype(BF16)
    loads[2].wait()

    def load_w(n, carry):
        for f in range(8):
            p = place_of(f)
            for half, w in enumerate((g_h, u_h)):
                pltpu.make_async_copy(
                    w.at[f * SL : (f + 1) * SL, cols(n, 128)],
                    wgu.at[n, p * SL : (p + 1) * SL, half * 128 : (half + 1) * 128],
                    wsem.at[0],
                ).start()
        return carry

    lax.fori_loop(0, NT, load_w, 0)
    for f in range(8):
        pltpu.make_async_copy(
            d_h.at[:, f * SL : (f + 1) * SL],
            dv.at[place_of(f) // 2, :, (place_of(f) % 2) * SL : (place_of(f) % 2 + 1) * SL],
            wsem.at[1],
        ).start()

    def term(dx, dc):
        part = up_v[:, cols(aa_at(dx, dc), SL)]
        return 2.0 * jnp.dot(rank, part, preferred_element_type=F32)

    ORDER = (2, 1, 3, 0)
    for dx in ORDER:
        lsend[dx] = term(dx, 1).astype(BF16)

    pl.semaphore_wait(barrier, 22)
    lc = [rcopy(lsend.at[i], lrecv.at[i], l_s.at[i], l_r.at[i], sib, ba) for i in range(4)]
    tc = [
        rcopy(tsend.at[i], trecv.at[i], t_s.at[i], t_r.at[i], aa_at(i, 0), ba)
        for i in range(1, 4)
    ]
    for dx in ORDER:
        lc[dx].start()

    loads[7].wait()
    ex0, ex1 = ex_ref[0:1, :], ex_ref[1:2, :]
    e_sub = lax.broadcasted_iota(jnp.int32, (E, TOK), 0)
    hit0, hit1 = ex0 == e_sub, ex1 == e_sub
    hit = hit0 | hit1
    earlier = (sub < lane).astype(BF16)
    pos = jnp.dot(hit.astype(BF16), earlier, preferred_element_type=F32)
    pos = jnp.where(hit, pos, -1.0)
    posx = jnp.concatenate(
        [jnp.broadcast_to(pos[e : e + 1, :], (CR, TOK)) for e in range(E)], axis=0
    )
    row16 = (sub % CR).astype(F32)
    picks = [(posx == row16 + float(CR * c)).astype(BF16) for c in range(CH)]

    own_term = None
    for dx in ORDER:
        t = term(dx, 0)
        lc[dx].wait_recv()
        t = t + lrecv[dx].astype(F32)
        if dx:
            tsend[dx] = t.astype(BF16)
            tc[dx - 1].start()
        else:
            own_term = t

    def id_copy(d):
        return rcopy(idrow_ref, ids.at[d], id_s.at[0], id_r.at[0], aa, ba_at(d))

    each_peer(lambda d: id_copy(d).start())
    ids[0] = idrow_ref[...]

    for c in loads[4:7]:
        c.wait()
    res = stream_v[...].astype(F32) + own_term
    for c in (1, 3, 2):
        tc[c - 1].wait_recv()
        res = res + trecv[c].astype(F32)
    resid[...] = res
    gain = gain_ref[...]
    sq = jnp.sum(res * res, axis=1, keepdims=True)
    stat_own[...] = jnp.transpose(jnp.broadcast_to(sq, (TOK, 128)))[0:8, :]
    stc = [
        rcopy(stat_own, stats.at[k], st_s.at[0], st_r.at[0], aa_at(k // 2, k % 2), ba)
        for k in range(1, 8)
    ]
    for c in stc:
        c.start()
    own_n = (res * gain).astype(BF16)
    nrm[xh] = own_n
    ncopy = rcopy(nrm.at[xh], nrm.at[xh], n_s.at[0], n_r.at[0], opp, ba)
    ncopy.start()

    grp = xp * 2 + core

    def a_copy(c, d):
        to = ba_at(d)
        return rcopy(
            outb.at[c, cols(div(to, 2), CR), cols(xh, SL)],
            xb.at[c, cols(ba, CR), cols(grp * 2 + xh, SL)],
            a_s.at[c, 0], a_r.at[c, 0], aa, to,
        )

    def o_copy(c, d):
        to = ba_at(d)
        return rcopy(
            outb.at[c, cols(div(to, 2), CR), cols(1 - xh, SL)],
            xb.at[c, cols(ba, CR), cols(grp * 2 + 1 - xh, SL)],
            a_s.at[c, 1], a_r.at[c, 1], aa, to,
        )

    def w_copy(c, d):
        to = ba_at(d)
        return rcopy(
            outb.at[c, cols(div(to, 2), CR), :],
            xb.at[c, cols(ba, CR), cols(grp, 2 * SL)],
            a_s.at[c, 0], a_r.at[c, 0], aa, to,
        )

    def fill(c, half):
        outb[c, :, cols(half, SL)] = jnp.dot(
            picks[c], nrm[half], preferred_element_type=F32
        ).astype(BF16)

    def send_rows(copy, c, at, width):
        each_peer(lambda d: copy(c, d).start())
        xb[c, cols(ba, CR), cols(grp * (2 * SL // width) + at, width)] = outb[
            c, cols(div(ba, 2), CR), cols(at, width)
        ]

    fill(0, xh)
    send_rows(a_copy, 0, xh, SL)
    total = stat_own[...]
    take(stats.at[pl.ds(1, 7)], st_r.at[0])
    for k in range(1, 8):
        total = total + stats[k]
    inv_row = lax.rsqrt(total * (1.0 / DIM) + EPS)

    e_row = lax.broadcasted_iota(jnp.int32, (8, TOK), 0)
    for e in range(E):
        rout[e] = jnp.where(e_row == 0, jnp.broadcast_to(pos[e : e + 1, :], (8, TOK)), inv_row)

    def rt_copy(d):
        to = ba_at(d)
        return rcopy(rout.at[div(to, 2)], routes.at[ba], rt_s.at[0], rt_r.at[0], aa, to)

    each_peer(lambda d: rt_copy(d).start())
    routes[ba] = rout[div(ba, 2)]
    fill(1, xh)
    send_rows(a_copy, 1, xh, SL)
    fill(2, xh)

    place = grp * 2 + xh
    xc, dc = [], []
    for c in range(CH):
        own = xb.at[c, :, cols(place, SL)]
        far = xb.at[c, :, cols(grp * 2 + 1 - xh, SL)]
        mine = xb.at[c, :, cols(grp, 2 * SL)]
        side = xb.at[c, :, cols((1 - xp) * 2 + core, 2 * SL)]
        xc.append(
            [
                rcopy(own, own, x_s.at[c, 0], x_r.at[c, 0], aa_at(1, 0), ba),
                rcopy(own, own, x_s.at[c, 1], x_r.at[c, 1], aa_at(3, 0), ba),
            ]
        )
        dc.append(
            [
                rcopy(r, r, d_s.at[c, i], d_r.at[c, i], sib, ba)
                for i, r in enumerate((own, far, side) if c < 2 else (mine, side))
            ]
        )

    quarter_ret = ret.at[0, pl.ds(0, ROWS - CR), pl.ds(0, HS)]
    half_ret = ret.at[0, pl.ds(0, ROWS - CR), pl.ds(0, SL)]
    half_rows = xb.at[0, pl.ds(0, ROWS - CR), pl.ds(0, SL)]
    full_rows = xb.at[0, pl.ds(0, ROWS - CR), pl.ds(0, 2 * SL)]

    def cross(c):
        for k in xc[c]:
            k.start()

    def arrive_own(c):
        take(half_rows, a_r.at[c, 0])
        if c == 0:
            cross(c)
        dc[c][0].start()

    def arrive_opp(c):
        take(half_rows, a_r.at[c, 1])
        dc[c][1].start()

    def arrive(c):
        take(full_rows, a_r.at[c, 0])
        for k in xc[c]:
            k.start()
        dc[c][0].start()

    def relay(c):
        for k in xc[c]:
            k.wait_recv()
        dc[c][-1].start()

    def scales(c):
        for s in range(16):
            r = routes[s]
            at = lax.broadcasted_iota(jnp.int32, (CR, TOK), 0).astype(F32) + float(CR * c)
            v = jnp.where(at == r[0:1, :], r[1:2, :], 0.0)
            scl[s * CR : (s + 1) * CR, :] = jnp.broadcast_to(
                jnp.sum(v, axis=1, keepdims=True), (CR, 128)
            )

    def activate(n, gu):
        g, u = gu[:, :128] * scl[...], gu[:, 128:] * scl[...]
        hid[:, n * 128 : (n + 1) * 128] = (g / (1.0 + jnp.exp(-g)) * u).astype(BF16)

    def part(n, *blocks):
        return sum(
            jnp.dot(xb[0, :, k], wgu[n, k, :], preferred_element_type=F32) for k in blocks
        )

    def gate_up(c):
        for n in range(NT):
            if n == 6 and c == 2:
                reduce_chips(0)
            activate(n, jnp.dot(xb[c], wgu[n], preferred_element_type=F32))

    def z_copy(c, dx, h):
        half, i = div(rem(x + dx, 4), 2), dx // 2
        return rcopy(
            zsend.at[c, :, cols(half * 2 + h, HS)], zrecv.at[c, i, :, h * HS : (h + 1) * HS],
            z_s.at[c, i + 2 * h], z_r.at[c, i + 2 * h], aa_at(dx, 0), ba,
        )

    zc = [[[z_copy(c, dx, h) for dx in (1, 3)] for h in range(2)] for c in range(CH)]
    yc = [
        [rcopy(ysend.at[c, i], yrecv.at[c, i], y_s.at[c, i], y_r.at[c, i], sib, ba) for i in range(2)]
        for c in range(CH)
    ]

    def b_copy(c, d, h):
        to = ba_at(d)
        at = cols(xh * 2 + h, HS)
        return rcopy(
            rb.at[c, cols(to, CR), at], ret.at[c, cols(ba, CR), at],
            b_s.at[c, h], b_r.at[c, h], aa, to,
        )

    def q_copy(c, d):
        to = ba_at(d)
        return rcopy(
            rb.at[c, cols(to, CR), cols(1 - xh, SL)], ret.at[c, cols(ba, CR), cols(1 - xh, SL)],
            b_s.at[c, 2], b_r.at[c, 2], aa, to,
        )

    def down(group):
        return jnp.dot(hid[...], dv[group], preferred_element_type=F32)

    def project(c, before_last):
        ysend[c, 0] = down((1 - xp) * 2 + 1 - core).astype(BF16)
        yc[c][0].start()
        ysend[c, 1] = down(xp * 2 + 1 - core).astype(BF16)
        yc[c][1].start()
        near[...] = down((1 - xp) * 2 + core)
        before_last()
        town[c] = down(xp * 2 + core)

    def pair_near(c):
        yc[c][0].wait_recv()
        zsend[c] = (near[...] + yrecv[c, 0].astype(F32)).astype(BF16)

    def pair_own(c):
        yc[c][1].wait_recv()
        v = town[c] + yrecv[c, 1].astype(F32)
        town[c] = v
        rb[c] = v.astype(BF16)

    def send_near(c):
        for k in zc[c][0] + zc[c][1]:
            k.start()

    def send_far(c):
        each_peer(lambda d: q_copy(c, d).start())
        ret[c, cols(ba, CR), cols(1 - xh, SL)] = rb[c, cols(ba, CR), cols(1 - xh, SL)]

    def reduce_chips(c):
        for h in range(2):
            for k in zc[c][h]:
                k.wait_recv()
            at, here = cols(xh * 2 + h, HS), slice(h * HS, (h + 1) * HS)
            rb[c, :, at] = (
                town[c, :, at] + zrecv[c, 0, :, here].astype(F32) + zrecv[c, 1, :, here].astype(F32)
            ).astype(BF16)
            each_peer(lambda d: b_copy(c, d, h).start())
            ret[c, cols(ba, CR), at] = rb[c, cols(ba, CR), at]

    def mix_weights():
        lg = lg_own[...]
        take(lgs.at[pl.ds(1, 7)], lg_r.at[0])
        for k in range(1, 8):
            lg = lg + lgs[k]
        l0 = jnp.sum(jnp.where(hit0, lg, 0.0), axis=0, keepdims=True)
        l1 = jnp.sum(jnp.where(hit1, lg, 0.0), axis=0, keepdims=True)
        w0 = 1.0 / (1.0 + jnp.exp(l1 - l0))
        w1 = 1.0 / (1.0 + jnp.exp(l0 - l1))
        return jnp.where(hit0, w0, 0.0) + jnp.where(hit1, w1, 0.0)

    def spread_weights(c, wx):
        w = jnp.where(posx == row16 + float(CR * c), wx, 0.0)
        hi = w.astype(BF16)
        lo = (w - hi.astype(F32)).astype(BF16)
        both = jnp.concatenate([hi, lo], axis=1)
        return jnp.concatenate(
            [both[(s // 2) * CR : (s // 2 + 1) * CR, :] for s in range(2 * E)], axis=0
        )

    def mix(c, wx, half):
        got = tdot(spread_weights(c, wx), ret[c, :, cols(half, SL)])
        got = got[:TOK, :] + got[TOK:, :]
        if c == 0:
            mx[half] = got
        else:
            mx[half] += got

    ncopy.wait_recv()
    fill(0, 1 - xh)
    send_rows(o_copy, 0, 1 - xh, SL)
    arrive_own(0)
    fill(1, 1 - xh)
    send_rows(o_copy, 1, 1 - xh, SL)
    fill(2, 1 - xh)
    inv = jnp.transpose(jnp.broadcast_to(inv_row[0:1, :], (128, TOK)))[:, 0:1]
    normed = (resid[...] * inv * gain).astype(BF16)
    lg_own[...] = ntdot(router_ref[...], normed)
    lgc = [
        rcopy(lg_own, lgs.at[k], lg_s.at[0], lg_r.at[0], aa_at(k // 2, k % 2), ba)
        for k in range(1, 8)
    ]
    for c in lgc:
        c.start()
    own_k = (cols(xp * 4 + xh, SL), cols(xp * 4 + 2 + xh, SL))
    far_k = (cols(xp * 4 + 1 - xh, SL), cols(xp * 4 + 3 - xh, SL))
    dc[0][0].wait_recv()
    pltpu.make_async_copy(wgu, wgu, wsem.at[0]).wait()
    for n in range(NT):
        acc[n] = part(n, *own_k)
    arrive_own(1)
    cross(1)
    take(routes.at[pl.ds(0, 15)], rt_r.at[0])
    scales(0)
    send_rows(w_copy, 2, 0, 2 * SL)
    arrive_opp(0)
    relay(0)
    dc[0][1].wait_recv()
    for n in range(NT):
        acc[n] += part(n, *far_k)
    arrive_opp(1)
    dc[0][2].wait_recv()
    for n in range(NT):
        activate(n, acc[n] + part(n, cols(1 - xp, 2048)))
    pltpu.make_async_copy(dv, dv, wsem.at[1]).wait()
    project(0, lambda: (relay(1), arrive(2)))
    pair_near(0)
    send_near(0)
    pair_own(0)
    send_far(0)
    scales(1)
    for k in dc[1]:
        k.wait_recv()
    gate_up(1)
    project(1, lambda: relay(2))
    pair_near(1)
    send_near(1)
    pair_own(1)
    send_far(1)
    scales(2)
    for k in dc[2][:2]:
        k.wait_recv()
    gate_up(2)
    wt = mix_weights()
    wx = jnp.concatenate(
        [jnp.broadcast_to(wt[e : e + 1, :], (CR, TOK)) for e in range(E)], axis=0
    )
    project(2, lambda: (pair_near(2), send_near(2)))
    pair_own(2)
    send_far(2)
    reduce_chips(1)
    take(ids.at[pl.ds(1, 15)], id_r.at[0])
    want = aa * 8 + lax.broadcasted_iota(jnp.int32, (8, TOK), 0)
    tally = jnp.zeros((8, TOK), F32)
    for d in range(16):
        tally = tally + (jnp.broadcast_to(ids[d], (8, TOK)) == want).astype(F32)
    cnt_ref[...] = jnp.broadcast_to(jnp.sum(tally, axis=1, keepdims=True), (8, TOK))

    for c in (0, 1):
        take(half_ret, b_r.at[c, 2])
        mix(c, wx, 1 - xh)
    take(quarter_ret, b_r.at[0, 0])
    take(quarter_ret, b_r.at[0, 1])
    mix(0, wx, xh)
    reduce_chips(2)
    take(half_ret, b_r.at[2, 2])
    mix(2, wx, 1 - xh)
    fsend[...] = mx[1 - xh].astype(BF16)
    fcopy = rcopy(fsend, frecv, f_s.at[0], f_r.at[0], opp, ba)
    fcopy.start()
    take(quarter_ret, b_r.at[1, 0])
    take(quarter_ret, b_r.at[1, 1])
    mix(1, wx, xh)
    take(quarter_ret, b_r.at[2, 0])
    take(quarter_ret, b_r.at[2, 1])
    mix(2, wx, xh)
    base = resid[...] + mx[xh]
    fcopy.wait_recv()
    out_ref[...] = (base + frecv[...].astype(F32)).astype(BF16)

    for c in lc + tc + [ncopy, fcopy]:
        c.wait_send()
    take(ids.at[pl.ds(1, 15)], id_s.at[0])
    take(stats.at[pl.ds(1, 7)], st_s.at[0])
    take(lgs.at[pl.ds(1, 7)], lg_s.at[0])
    take(routes.at[pl.ds(0, 15)], rt_s.at[0])
    for c in range(2):
        take(half_rows, a_s.at[c, 0])
        take(half_rows, a_s.at[c, 1])
    take(full_rows, a_s.at[2, 0])
    for c in range(CH):
        take(quarter_ret, b_s.at[c, 0])
        take(quarter_ret, b_s.at[c, 1])
        take(half_ret, b_s.at[c, 2])
    for c in range(CH):
        for k in xc[c] + zc[c][0] + zc[c][1] + dc[c] + yc[c]:
            k.wait_send()


def shards(
    head_outputs, stream, adapter_down_factors, adapter_up_factors, norm_gain_vector,
    router_matrix, token_adapter_index, token_expert_index, gate_weight, up_weight, down_weight,
):
    hbm = pl.BlockSpec(memory_space=pltpu.HBM)
    vmem = pl.BlockSpec(memory_space=pltpu.VMEM)
    V = pltpu.VMEM
    S = pltpu.SemaphoreType.DMA
    mixed, load = pl.pallas_call(
        kernel,
        out_shape=(
            jax.ShapeDtypeStruct((TOK, SL), BF16),
            jax.ShapeDtypeStruct((8, TOK), F32),
        ),
        in_specs=[hbm] * 11,
        out_specs=(vmem, vmem),
        scratch_shapes=[
            V((TOK, DIM), BF16),
            V((DIM, 128), BF16),
            V((128, DIM), BF16),
            V((TOK, SL), BF16),
            V((1, SL), F32),
            V((E, SL), BF16),
            V((1, TOK), jnp.int32),
            V((2, TOK), jnp.int32),
            V((NT, DIM, 256), BF16),
            V((4, FFD, 2 * SL), BF16),
            V((4, TOK, SL), BF16),
            V((4, TOK, SL), BF16),
            V((4, TOK, SL), BF16),
            V((4, TOK, SL), BF16),
            V((8, 8, TOK), F32),
            V((8, TOK), F32),
            V((8, E, TOK), F32),
            V((E, TOK), F32),
            V((16, 1, TOK), jnp.int32),
            V((E, 8, TOK), F32),
            V((16, 8, TOK), F32),
            V((ROWS, 128), F32),
            V((2, TOK, SL), BF16),
            V((CH, E * CR, 2 * SL), BF16),
            V((CH, ROWS, DIM), BF16),
            V((ROWS, FFD), BF16),
            V((CH, 2, ROWS, 2 * SL), BF16),
            V((CH, 2, ROWS, 2 * SL), BF16),
            V((ROWS, 2 * SL), F32),
            V((CH, ROWS, 2 * SL), F32),
            V((CH, ROWS, 2 * SL), BF16),
            V((CH, 2, ROWS, SL), BF16),
            V((CH, ROWS, 2 * SL), BF16),
            V((CH, ROWS, 2 * SL), BF16),
            V((2, TOK, SL), F32),
            V((TOK, SL), BF16),
            V((TOK, SL), BF16),
            V((TOK, SL), F32),
            V((NT, ROWS, 256), F32),
            S((8,)), S((2,)),
            S((4,)), S((4,)), S((4,)), S((4,)), S((1,)), S((1,)), S((1,)), S((1,)),
            S((1,)), S((1,)), S((1,)), S((1,)),
            S((1,)), S((1,)),
            S((CH, 2)), S((CH, 2)),
            S((CH, 2)), S((CH, 2)), S((CH, 3)), S((CH, 3)),
            S((CH, 2)), S((CH, 2)),
            S((CH, 4)), S((CH, 4)),
            S((CH, 3)), S((CH, 3)),
            S((1,)), S((1,)),
        ],
        compiler_params=pltpu.CompilerParams(
            collective_id=0, has_side_effects=True, vmem_limit_bytes=56_000_000
        ),
    )(*[pltpu.with_memory_space_constraint(a, pltpu.HBM) for a in (
        head_outputs, stream, adapter_down_factors, adapter_up_factors,
        norm_gain_vector.reshape(1, DIM), router_matrix.T,
        token_adapter_index.reshape(1, TOK),
        token_expert_index.T, gate_weight[0], up_weight[0], down_weight[0],
    )])
    return mixed, load[:, 0]


def solution(mesh):
    in_specs = (
        P("ba", None), P("ba", None), P(None, "aa"), P("aa", None), P(), P(), P("ba"),
        P("ba", None), P("ba", None, "aa"), P("ba", None, "aa"), P("ba", "aa", None),
    )
    out_specs = (P("ba", "aa"), P("aa"))
    return jax.shard_map(shards, mesh=mesh, in_specs=in_specs, out_specs=out_specs, check_vma=False)
```

```python
import jax
import jax.numpy as jnp
from jax import lax
from jax.experimental import pallas as pl
from jax.experimental.pallas import tpu as pltpu
from jax.sharding import PartitionSpec as P

MESH = pl.DeviceIdType.MESH
E = 8
RANK = 16
TOK = 128
DIM = 4096
FFD = 896
CH = 3
CR = 16
ROWS = 256
SL = 512
HS = SL // 2
NT = FFD // 128
EPS = 1e-05
F32 = jnp.float32
BF16 = jnp.bfloat16


def place_of(f):
    x, core = f // 2, f % 2
    return (x % 2) * 4 + core * 2 + x // 2


def tdot(a, b):
    return lax.dot_general(a, b, (((0,), (0,)), ((), ())), preferred_element_type=F32)


def ntdot(a, b):
    return lax.dot_general(a, b, (((1,), (1,)), ((), ())), preferred_element_type=F32)


def kernel(
    head_h, stream_h, down_h, up_h, gain_h, router_h, idrow_h, ex_h,
    g_h, u_h, d_h,
    out_ref, cnt_ref,
    head_v, down_v, up_v, stream_v, gain_ref, router_ref, idrow_ref, ex_ref, wgu, dv, lsend, lrecv, tsend, trecv, stats, stat_own,
    lgs, lg_own, ids, rout, routes, scl,
    nrm, outb, xb, hid, ysend, yrecv, near, town, zsend, zrecv, rb, ret, mx, fsend, frecv, resid, acc,
    load_sem, wsem, l_s, l_r, t_s, t_r, st_s, st_r, lg_s, lg_r, id_s, id_r, rt_s, rt_r,
    n_s, n_r, a_s, a_r, x_s, x_r, d_s, d_r, y_s, y_r, z_s, z_r,
    b_s, b_r, f_s, f_r,
):
    aa = lax.axis_index("aa")
    ba = lax.axis_index("ba")
    rem, div = lax.rem, lax.div
    core, x = rem(aa, 2), div(aa, 2)
    xp, xh = rem(x, 2), div(x, 2)
    z, y = div(ba, 4), rem(ba, 4)

    def aa_at(dx, dc):
        return rem(x + dx, 4) * 2 + rem(core + dc, 2)

    peers = [rem(z + d // 4, 4) * 4 + rem(y + d % 4, 4) for d in range(16)]

    def ba_at(d):
        return peers[d]

    def take(ref, sem):
        pltpu.make_async_copy(ref, ref, sem).wait()

    def rcopy(src, dst, ss, rs, a, b):
        return pltpu.make_async_remote_copy(
            src_ref=src, dst_ref=dst, send_sem=ss, recv_sem=rs, device_id=(a, b),
            device_id_type=MESH,
        )

    def cols(i, width):
        return pl.ds(pl.multiple_of(i * width, width), width)

    def each_peer(body):
        for d in range(1, 16):
            body(d)

    sib = aa_at(0, 1)
    opp = aa_at(2, 0)

    loads = [
        pltpu.make_async_copy(head_h, head_v, load_sem.at[0]),
        pltpu.make_async_copy(down_h, down_v, load_sem.at[1]),
        pltpu.make_async_copy(up_h, up_v, load_sem.at[2]),
        pltpu.make_async_copy(idrow_h, idrow_ref, load_sem.at[4]),
        pltpu.make_async_copy(stream_h.at[:, cols(aa, SL)], stream_v, load_sem.at[3]),
        pltpu.make_async_copy(gain_h.at[:, cols(aa, SL)], gain_ref, load_sem.at[5]),
        pltpu.make_async_copy(router_h.at[:, cols(aa, SL)], router_ref, load_sem.at[6]),
        pltpu.make_async_copy(ex_h, ex_ref, load_sem.at[7]),
    ]
    for c in loads:
        c.start()

    barrier = pltpu.get_barrier_semaphore()
    for k in range(1, 8):
        pl.semaphore_signal(
            barrier, inc=1, device_id=(aa_at(k // 2, k % 2), ba), device_id_type=MESH
        )
    each_peer(
        lambda d: pl.semaphore_signal(
            barrier, inc=1, device_id=(aa, ba_at(d)), device_id_type=MESH
        )
    )

    lane = lax.broadcasted_iota(jnp.int32, (TOK, 128), 1)
    sub = lax.broadcasted_iota(jnp.int32, (TOK, 128), 0)
    loads[0].wait()
    loads[1].wait()
    loads[3].wait()
    rank = jnp.dot(head_v[...], down_v[...], preferred_element_type=F32)
    idcol = jnp.transpose(jnp.broadcast_to(idrow_ref[...].astype(F32), (128, TOK)))
    rank = jnp.where(idcol == (aa * 8 + lane // RANK).astype(F32), rank, 0.0).astype(BF16)
    loads[2].wait()

    def term(dx, dc):
        part = up_v[:, cols(aa_at(dx, dc), SL)]
        return 2.0 * jnp.dot(rank, part, preferred_element_type=F32)

    ORDER = (2, 1, 3, 0)
    for dx in ORDER:
        lsend[dx] = term(dx, 1).astype(BF16)

    pl.semaphore_wait(barrier, 22)
    lc = [rcopy(lsend.at[i], lrecv.at[i], l_s.at[i], l_r.at[i], sib, ba) for i in range(4)]
    tc = [
        rcopy(tsend.at[i], trecv.at[i], t_s.at[i], t_r.at[i], aa_at(i, 0), ba)
        for i in range(1, 4)
    ]
    for dx in ORDER:
        lc[dx].start()

    own_term = None
    for dx in ORDER:
        t = term(dx, 0)
        lc[dx].wait_recv()
        t = t + lrecv[dx].astype(F32)
        if dx:
            tsend[dx] = t.astype(BF16)
            tc[dx - 1].start()
        else:
            own_term = t

    def load_w(n, carry):
        for f in range(8):
            p = place_of(f)
            for half, w in enumerate((g_h, u_h)):
                pltpu.make_async_copy(
                    w.at[f * SL : (f + 1) * SL, cols(n, 128)],
                    wgu.at[n, p * SL : (p + 1) * SL, half * 128 : (half + 1) * 128],
                    wsem.at[0],
                ).start()
        return carry

    lax.fori_loop(0, NT, load_w, 0)
    for f in range(8):
        pltpu.make_async_copy(
            d_h.at[:, f * SL : (f + 1) * SL],
            dv.at[place_of(f) // 2, :, (place_of(f) % 2) * SL : (place_of(f) % 2 + 1) * SL],
            wsem.at[1],
        ).start()

    def id_copy(d):
        return rcopy(idrow_ref, ids.at[d], id_s.at[0], id_r.at[0], aa, ba_at(d))

    each_peer(lambda d: id_copy(d).start())
    ids[0] = idrow_ref[...]

    loads[7].wait()
    ex0, ex1 = ex_ref[0:1, :], ex_ref[1:2, :]
    e_sub = lax.broadcasted_iota(jnp.int32, (E, TOK), 0)
    hit0, hit1 = ex0 == e_sub, ex1 == e_sub
    hit = hit0 | hit1
    earlier = (sub < lane).astype(BF16)
    pos = jnp.dot(hit.astype(BF16), earlier, preferred_element_type=F32)
    pos = jnp.where(hit, pos, -1.0)
    posx = jnp.concatenate(
        [jnp.broadcast_to(pos[e : e + 1, :], (CR, TOK)) for e in range(E)], axis=0
    )
    row16 = (sub % CR).astype(F32)
    picks = [(posx == row16 + float(CR * c)).astype(BF16) for c in range(CH)]

    for c in loads[4:7]:
        c.wait()
    res = stream_v[...].astype(F32) + own_term
    for c in (1, 3, 2):
        tc[c - 1].wait_recv()
        res = res + trecv[c].astype(F32)
    resid[...] = res
    gain = gain_ref[...]
    own_n = (res * gain).astype(BF16)
    nrm[xh] = own_n
    ncopy = rcopy(nrm.at[xh], nrm.at[xh], n_s.at[0], n_r.at[0], opp, ba)
    ncopy.start()

    grp = xp * 2 + core

    def a_copy(c, d):
        to = ba_at(d)
        return rcopy(
            outb.at[c, cols(div(to, 2), CR), cols(xh, SL)],
            xb.at[c, cols(ba, CR), cols(grp * 2 + xh, SL)],
            a_s.at[c, 0], a_r.at[c, 0], aa, to,
        )

    def o_copy(c, d):
        to = ba_at(d)
        return rcopy(
            outb.at[c, cols(div(to, 2), CR), cols(1 - xh, SL)],
            xb.at[c, cols(ba, CR), cols(grp * 2 + 1 - xh, SL)],
            a_s.at[c, 1], a_r.at[c, 1], aa, to,
        )

    def w_copy(c, d):
        to = ba_at(d)
        return rcopy(
            outb.at[c, cols(div(to, 2), CR), :],
            xb.at[c, cols(ba, CR), cols(grp, 2 * SL)],
            a_s.at[c, 0], a_r.at[c, 0], aa, to,
        )

    def fill(c, half):
        outb[c, :, cols(half, SL)] = jnp.dot(
            picks[c], nrm[half], preferred_element_type=F32
        ).astype(BF16)

    def send_rows(copy, c, at, width):
        each_peer(lambda d: copy(c, d).start())
        xb[c, cols(ba, CR), cols(grp * (2 * SL // width) + at, width)] = outb[
            c, cols(div(ba, 2), CR), cols(at, width)
        ]

    fill(0, xh)
    send_rows(a_copy, 0, xh, SL)
    sq = jnp.sum(res * res, axis=1, keepdims=True)
    stat_own[...] = jnp.transpose(jnp.broadcast_to(sq, (TOK, 128)))[0:8, :]
    stc = [
        rcopy(stat_own, stats.at[k], st_s.at[0], st_r.at[0], aa_at(k // 2, k % 2), ba)
        for k in range(1, 8)
    ]
    for c in stc:
        c.start()
    fill(1, xh)
    send_rows(a_copy, 1, xh, SL)
    fill(2, xh)

    place = grp * 2 + xh
    xc, dc = [], []
    for c in range(CH):
        own = xb.at[c, :, cols(place, SL)]
        far = xb.at[c, :, cols(grp * 2 + 1 - xh, SL)]
        mine = xb.at[c, :, cols(grp, 2 * SL)]
        side = xb.at[c, :, cols((1 - xp) * 2 + core, 2 * SL)]
        xc.append(
            [
                rcopy(own, own, x_s.at[c, 0], x_r.at[c, 0], aa_at(1, 0), ba),
                rcopy(own, own, x_s.at[c, 1], x_r.at[c, 1], aa_at(3, 0), ba),
            ]
        )
        dc.append(
            [
                rcopy(r, r, d_s.at[c, i], d_r.at[c, i], sib, ba)
                for i, r in enumerate((own, far, side) if c < 2 else (mine, side))
            ]
        )

    quarter_ret = ret.at[0, pl.ds(0, ROWS - CR), pl.ds(0, HS)]
    half_ret = ret.at[0, pl.ds(0, ROWS - CR), pl.ds(0, SL)]
    half_rows = xb.at[0, pl.ds(0, ROWS - CR), pl.ds(0, SL)]
    full_rows = xb.at[0, pl.ds(0, ROWS - CR), pl.ds(0, 2 * SL)]

    def cross(c):
        for k in xc[c]:
            k.start()

    def arrive_own(c):
        take(half_rows, a_r.at[c, 0])
        if c == 0:
            cross(c)
        dc[c][0].start()

    def arrive_opp(c):
        take(half_rows, a_r.at[c, 1])
        dc[c][1].start()

    def arrive(c):
        take(full_rows, a_r.at[c, 0])
        for k in xc[c]:
            k.start()
        dc[c][0].start()

    def relay(c):
        for k in xc[c]:
            k.wait_recv()
        dc[c][-1].start()

    def scales(c):
        for s in range(16):
            r = routes[s]
            at = lax.broadcasted_iota(jnp.int32, (CR, TOK), 0).astype(F32) + float(CR * c)
            v = jnp.where(at == r[0:1, :], r[1:2, :], 0.0)
            scl[s * CR : (s + 1) * CR, :] = jnp.broadcast_to(
                jnp.sum(v, axis=1, keepdims=True), (CR, 128)
            )

    def activate(n, gu):
        g, u = gu[:, :128] * scl[...], gu[:, 128:] * scl[...]
        hid[:, n * 128 : (n + 1) * 128] = (g / (1.0 + jnp.exp(-g)) * u).astype(BF16)

    def part(n, *blocks):
        return sum(
            jnp.dot(xb[0, :, k], wgu[n, k, :], preferred_element_type=F32) for k in blocks
        )

    def gate_up(c):
        for n in range(NT):
            if n == 6 and c == 2:
                reduce_chips(0)
            activate(n, jnp.dot(xb[c], wgu[n], preferred_element_type=F32))

    def z_copy(c, dx, h):
        half, i = div(rem(x + dx, 4), 2), dx // 2
        return rcopy(
            zsend.at[c, :, cols(half * 2 + h, HS)], zrecv.at[c, i, :, h * HS : (h + 1) * HS],
            z_s.at[c, i + 2 * h], z_r.at[c, i + 2 * h], aa_at(dx, 0), ba,
        )

    zc = [[[z_copy(c, dx, h) for dx in (1, 3)] for h in range(2)] for c in range(CH)]
    yc = [
        [rcopy(ysend.at[c, i], yrecv.at[c, i], y_s.at[c, i], y_r.at[c, i], sib, ba) for i in range(2)]
        for c in range(CH)
    ]

    def b_copy(c, d, h):
        to = ba_at(d)
        at = cols(xh * 2 + h, HS)
        return rcopy(
            rb.at[c, cols(to, CR), at], ret.at[c, cols(ba, CR), at],
            b_s.at[c, h], b_r.at[c, h], aa, to,
        )

    def q_copy(c, d):
        to = ba_at(d)
        return rcopy(
            rb.at[c, cols(to, CR), cols(1 - xh, SL)], ret.at[c, cols(ba, CR), cols(1 - xh, SL)],
            b_s.at[c, 2], b_r.at[c, 2], aa, to,
        )

    def down(group):
        return jnp.dot(hid[...], dv[group], preferred_element_type=F32)

    def project(c, before_last):
        ysend[c, 0] = down((1 - xp) * 2 + 1 - core).astype(BF16)
        yc[c][0].start()
        ysend[c, 1] = down(xp * 2 + 1 - core).astype(BF16)
        yc[c][1].start()
        near[...] = down((1 - xp) * 2 + core)
        before_last()
        town[c] = down(xp * 2 + core)

    def pair_near(c):
        yc[c][0].wait_recv()
        zsend[c] = (near[...] + yrecv[c, 0].astype(F32)).astype(BF16)

    def pair_own(c):
        yc[c][1].wait_recv()
        v = town[c] + yrecv[c, 1].astype(F32)
        town[c] = v
        rb[c] = v.astype(BF16)

    def send_near(c):
        for k in zc[c][0] + zc[c][1]:
            k.start()

    def send_far(c):
        each_peer(lambda d: q_copy(c, d).start())
        ret[c, cols(ba, CR), cols(1 - xh, SL)] = rb[c, cols(ba, CR), cols(1 - xh, SL)]

    def reduce_chips(c):
        for h in range(2):
            for k in zc[c][h]:
                k.wait_recv()
            at, here = cols(xh * 2 + h, HS), slice(h * HS, (h + 1) * HS)
            rb[c, :, at] = (
                town[c, :, at] + zrecv[c, 0, :, here].astype(F32) + zrecv[c, 1, :, here].astype(F32)
            ).astype(BF16)
            each_peer(lambda d: b_copy(c, d, h).start())
            ret[c, cols(ba, CR), at] = rb[c, cols(ba, CR), at]

    def mix_weights():
        lg = lg_own[...]
        take(lgs.at[pl.ds(1, 7)], lg_r.at[0])
        for k in range(1, 8):
            lg = lg + lgs[k]
        l0 = jnp.sum(jnp.where(hit0, lg, 0.0), axis=0, keepdims=True)
        l1 = jnp.sum(jnp.where(hit1, lg, 0.0), axis=0, keepdims=True)
        w0 = 1.0 / (1.0 + jnp.exp(l1 - l0))
        w1 = 1.0 / (1.0 + jnp.exp(l0 - l1))
        return jnp.where(hit0, w0, 0.0) + jnp.where(hit1, w1, 0.0)

    def spread_weights(c, wx):
        w = jnp.where(posx == row16 + float(CR * c), wx, 0.0)
        hi = w.astype(BF16)
        lo = (w - hi.astype(F32)).astype(BF16)
        both = jnp.concatenate([hi, lo], axis=1)
        return jnp.concatenate(
            [both[(s // 2) * CR : (s // 2 + 1) * CR, :] for s in range(2 * E)], axis=0
        )

    def mix(c, wx, half):
        got = tdot(spread_weights(c, wx), ret[c, :, cols(half, SL)])
        got = got[:TOK, :] + got[TOK:, :]
        if c == 0:
            mx[half] = got
        else:
            mx[half] += got

    ncopy.wait_recv()
    fill(0, 1 - xh)
    send_rows(o_copy, 0, 1 - xh, SL)
    arrive_own(0)
    total = stat_own[...]
    take(stats.at[pl.ds(1, 7)], st_r.at[0])
    for k in range(1, 8):
        total = total + stats[k]
    inv_row = lax.rsqrt(total * (1.0 / DIM) + EPS)

    e_row = lax.broadcasted_iota(jnp.int32, (8, TOK), 0)
    for e in range(E):
        rout[e] = jnp.where(e_row == 0, jnp.broadcast_to(pos[e : e + 1, :], (8, TOK)), inv_row)

    def rt_copy(d):
        to = ba_at(d)
        return rcopy(rout.at[div(to, 2)], routes.at[ba], rt_s.at[0], rt_r.at[0], aa, to)

    each_peer(lambda d: rt_copy(d).start())
    routes[ba] = rout[div(ba, 2)]
    fill(1, 1 - xh)
    send_rows(o_copy, 1, 1 - xh, SL)
    fill(2, 1 - xh)
    inv = jnp.transpose(jnp.broadcast_to(inv_row[0:1, :], (128, TOK)))[:, 0:1]
    normed = (resid[...] * inv * gain).astype(BF16)
    lg_own[...] = ntdot(router_ref[...], normed)
    lgc = [
        rcopy(lg_own, lgs.at[k], lg_s.at[0], lg_r.at[0], aa_at(k // 2, k % 2), ba)
        for k in range(1, 8)
    ]
    for c in lgc:
        c.start()
    own_k = (cols(xp * 4 + xh, SL), cols(xp * 4 + 2 + xh, SL))
    far_k = (cols(xp * 4 + 1 - xh, SL), cols(xp * 4 + 3 - xh, SL))
    dc[0][0].wait_recv()
    pltpu.make_async_copy(wgu, wgu, wsem.at[0]).wait()
    for n in range(NT):
        acc[n] = part(n, *own_k)
    arrive_own(1)
    cross(1)
    take(routes.at[pl.ds(0, 15)], rt_r.at[0])
    scales(0)
    send_rows(w_copy, 2, 0, 2 * SL)
    arrive_opp(0)
    relay(0)
    dc[0][1].wait_recv()
    for n in range(NT):
        acc[n] += part(n, *far_k)
    arrive_opp(1)
    dc[0][2].wait_recv()
    for n in range(NT):
        activate(n, acc[n] + part(n, cols(1 - xp, 2048)))
    pltpu.make_async_copy(dv, dv, wsem.at[1]).wait()
    project(0, lambda: (relay(1), arrive(2)))
    pair_near(0)
    send_near(0)
    pair_own(0)
    send_far(0)
    scales(1)
    for k in dc[1]:
        k.wait_recv()
    gate_up(1)
    project(1, lambda: relay(2))
    pair_near(1)
    send_near(1)
    pair_own(1)
    send_far(1)
    scales(2)
    for k in dc[2][:2]:
        k.wait_recv()
    gate_up(2)
    wt = mix_weights()
    wx = jnp.concatenate(
        [jnp.broadcast_to(wt[e : e + 1, :], (CR, TOK)) for e in range(E)], axis=0
    )
    project(2, lambda: (pair_near(2), send_near(2)))
    pair_own(2)
    send_far(2)
    reduce_chips(1)
    take(ids.at[pl.ds(1, 15)], id_r.at[0])
    want = aa * 8 + lax.broadcasted_iota(jnp.int32, (8, TOK), 0)
    tally = jnp.zeros((8, TOK), F32)
    for d in range(16):
        tally = tally + (jnp.broadcast_to(ids[d], (8, TOK)) == want).astype(F32)
    cnt_ref[...] = jnp.broadcast_to(jnp.sum(tally, axis=1, keepdims=True), (8, TOK))

    for c in (0, 1):
        take(half_ret, b_r.at[c, 2])
        mix(c, wx, 1 - xh)
    take(quarter_ret, b_r.at[0, 0])
    take(quarter_ret, b_r.at[0, 1])
    mix(0, wx, xh)
    reduce_chips(2)
    take(half_ret, b_r.at[2, 2])
    mix(2, wx, 1 - xh)
    fsend[...] = mx[1 - xh].astype(BF16)
    fcopy = rcopy(fsend, frecv, f_s.at[0], f_r.at[0], opp, ba)
    fcopy.start()
    take(quarter_ret, b_r.at[1, 0])
    take(quarter_ret, b_r.at[1, 1])
    mix(1, wx, xh)
    take(quarter_ret, b_r.at[2, 0])
    take(quarter_ret, b_r.at[2, 1])
    mix(2, wx, xh)
    base = resid[...] + mx[xh]
    fcopy.wait_recv()
    out_ref[...] = (base + frecv[...].astype(F32)).astype(BF16)

    for c in lc + tc + [ncopy, fcopy]:
        c.wait_send()
    take(ids.at[pl.ds(1, 15)], id_s.at[0])
    take(stats.at[pl.ds(1, 7)], st_s.at[0])
    take(lgs.at[pl.ds(1, 7)], lg_s.at[0])
    take(routes.at[pl.ds(0, 15)], rt_s.at[0])
    for c in range(2):
        take(half_rows, a_s.at[c, 0])
        take(half_rows, a_s.at[c, 1])
    take(full_rows, a_s.at[2, 0])
    for c in range(CH):
        take(quarter_ret, b_s.at[c, 0])
        take(quarter_ret, b_s.at[c, 1])
        take(half_ret, b_s.at[c, 2])
    for c in range(CH):
        for k in xc[c] + zc[c][0] + zc[c][1] + dc[c] + yc[c]:
            k.wait_send()


def shards(
    head_outputs, stream, adapter_down_factors, adapter_up_factors, norm_gain_vector,
    router_matrix, token_adapter_index, token_expert_index, gate_weight, up_weight, down_weight,
):
    hbm = pl.BlockSpec(memory_space=pltpu.HBM)
    vmem = pl.BlockSpec(memory_space=pltpu.VMEM)
    V = pltpu.VMEM
    S = pltpu.SemaphoreType.DMA
    mixed, load = pl.pallas_call(
        kernel,
        out_shape=(
            jax.ShapeDtypeStruct((TOK, SL), BF16),
            jax.ShapeDtypeStruct((8, TOK), F32),
        ),
        in_specs=[hbm] * 11,
        out_specs=(vmem, vmem),
        scratch_shapes=[
            V((TOK, DIM), BF16),
            V((DIM, 128), BF16),
            V((128, DIM), BF16),
            V((TOK, SL), BF16),
            V((1, SL), F32),
            V((E, SL), BF16),
            V((1, TOK), jnp.int32),
            V((2, TOK), jnp.int32),
            V((NT, DIM, 256), BF16),
            V((4, FFD, 2 * SL), BF16),
            V((4, TOK, SL), BF16),
            V((4, TOK, SL), BF16),
            V((4, TOK, SL), BF16),
            V((4, TOK, SL), BF16),
            V((8, 8, TOK), F32),
            V((8, TOK), F32),
            V((8, E, TOK), F32),
            V((E, TOK), F32),
            V((16, 1, TOK), jnp.int32),
            V((E, 8, TOK), F32),
            V((16, 8, TOK), F32),
            V((ROWS, 128), F32),
            V((2, TOK, SL), BF16),
            V((CH, E * CR, 2 * SL), BF16),
            V((CH, ROWS, DIM), BF16),
            V((ROWS, FFD), BF16),
            V((CH, 2, ROWS, 2 * SL), BF16),
            V((CH, 2, ROWS, 2 * SL), BF16),
            V((ROWS, 2 * SL), F32),
            V((CH, ROWS, 2 * SL), F32),
            V((CH, ROWS, 2 * SL), BF16),
            V((CH, 2, ROWS, SL), BF16),
            V((CH, ROWS, 2 * SL), BF16),
            V((CH, ROWS, 2 * SL), BF16),
            V((2, TOK, SL), F32),
            V((TOK, SL), BF16),
            V((TOK, SL), BF16),
            V((TOK, SL), F32),
            V((NT, ROWS, 256), F32),
            S((8,)), S((2,)),
            S((4,)), S((4,)), S((4,)), S((4,)), S((1,)), S((1,)), S((1,)), S((1,)),
            S((1,)), S((1,)), S((1,)), S((1,)),
            S((1,)), S((1,)),
            S((CH, 2)), S((CH, 2)),
            S((CH, 2)), S((CH, 2)), S((CH, 3)), S((CH, 3)),
            S((CH, 2)), S((CH, 2)),
            S((CH, 4)), S((CH, 4)),
            S((CH, 3)), S((CH, 3)),
            S((1,)), S((1,)),
        ],
        compiler_params=pltpu.CompilerParams(
            collective_id=0, has_side_effects=True, vmem_limit_bytes=56_000_000
        ),
    )(*[pltpu.with_memory_space_constraint(a, pltpu.HBM) for a in (
        head_outputs, stream, adapter_down_factors, adapter_up_factors,
        norm_gain_vector.reshape(1, DIM), router_matrix.T,
        token_adapter_index.reshape(1, TOK),
        token_expert_index.T, gate_weight[0], up_weight[0], down_weight[0],
    )])
    return mixed, load[:, 0]


def solution(mesh):
    in_specs = (
        P("ba", None), P("ba", None), P(None, "aa"), P("aa", None), P(), P(), P("ba"),
        P("ba", None), P("ba", None, "aa"), P("ba", None, "aa"), P("ba", "aa", None),
    )
    out_specs = (P("ba", "aa"), P("aa"))
    return jax.shard_map(shards, mesh=mesh, in_specs=in_specs, out_specs=out_specs, check_vma=False)
```
